128 devices in a mesh: row: 16 (over y_lo, x, core), col: 8 (over y_hi, z).
Axes of the slice: x: 4, y: 4 (y_hi: 2, y_lo: 2; y = y_hi * 2 + y_lo), z: 4, core: 2. Of those that a mesh axis runs over, the one named last changes fastest.
Arguments:
- tokens: bfloat16 [2048, 8192], P('row', 'col'), may hold values from -6 to 6
- weights: bfloat16 [2, 14336, 8192], P(None, 'row', 'col'), may hold values from -0.0625 to 0.0625
- gradients: bfloat16 [2, 14336, 8192], P(None, 'row', 'col'), may hold values from -200 to 200, as said below
- row_factors: float32 [2, 14336], P(None, 'row'), may hold values from 0.05 to 0.5
- col_factors: float32 [2, 8192], P(None, 'col'), may hold values from 0.05 to 0.5
Outputs:
- hidden: bfloat16 [2048, 14336], P('col', 'row')
- row_new: float32 [2, 14336], P(None, 'row')
- col_new: float32 [2, 8192], P(None, 'col')
The draws below stay inside these ranges and needn't reach their ends.
Inputs may be any that keep to these rules, and one draw needn't show every extreme that they name: Finite real gradients.
All inputs are finite; a program needn't handle non-finite values.
Results may differ from the reference program's by a relative error of at most 0.001.
The reference program's roundings to bfloat16 on the way (of `new_weights`) count: a program that leaves them out, or rounds other values in their place, can miss the bound.
Values may be sent and summed in bfloat16 or wider, within the bound.
A program may use at most 128 MiB of HBM per device.

```python
import math
import jax
import jax.numpy as jnp
from jax import lax

D = 8192
FF = 14336
TOKENS = 2048


def draw_gradients(key, part):
    keys = jax.random.split(jax.random.fold_in(key, 17), 5)
    row_pos = jnp.arange(FF, dtype=jnp.float32) / FF
    col_pos = jnp.arange(D, dtype=jnp.float32) / D
    row_scale = 0.5 * jnp.power(3.0, row_pos)[None, :, None] * jnp.exp(jax.random.uniform(keys[0], (2, FF, 1), jnp.float32, math.log(0.4), math.log(2.5)))
    col_scale = 0.5 * jnp.power(3.0, col_pos)[None, None, :] * jnp.exp(jax.random.uniform(keys[1], (2, 1, D), jnp.float32, math.log(0.4), math.log(2.5)))
    values = jax.random.normal(keys[4], (2, FF, D), jnp.float32) * row_scale * col_scale
    return jnp.clip(values, -200.0, 200.0).astype(jnp.bfloat16)


def block_levels(key, dims, shards, least, largest):
    gain = 1.0
    for dim, parts in shards:
        heights = jax.random.uniform(jax.random.fold_in(jax.random.fold_in(key, 6), dim), (parts,), jnp.float32, least / len(shards), largest / len(shards))
        gain = gain * jnp.repeat(jnp.exp(heights), dims[dim] // parts).reshape((-1,) + (1,) * (len(dims) - 1 - dim))
    return gain


def bell_draw(rng, shape, deviation, limit, cuts=(), kind=jnp.bfloat16):
    gain = block_levels(rng, shape, cuts, -0.22, 0.18) if cuts else 1.0
    values = jax.random.normal(rng, shape, jnp.float32) * deviation * gain
    return jnp.minimum(jnp.maximum(values, -limit), limit).astype(kind)


def setup_inputs(seed: int = 0) -> dict:
    key_list = jax.random.split(jax.random.key(seed), 6)
    return {
        "tokens": bell_draw(key_list[0], (TOKENS, D), 1.0, 6.0, ((0, 16), (1, 8))),
        "weights": bell_draw(key_list[1], (2, FF, D), D ** -0.5, 0.0625, ((1, 16), (2, 8))),
        "gradients": draw_gradients(jax.random.fold_in(key_list[5], 71), 0),
        "row_factors": jnp.clip(jnp.exp(math.log(0.5) - 2.3025851 * jax.random.uniform(key_list[3], (2, FF), jnp.float32) ** block_levels(key_list[3], (2, FF), ((1, 16),), -0.2, 0.2)), 0.05, 0.5),
        "col_factors": jnp.clip(jnp.exp(math.log(0.5) - 2.3025851 * jax.random.uniform(key_list[4], (2, D), jnp.float32) ** block_levels(key_list[4], (2, D), ((1, 8),), -0.2, 0.2)), 0.05, 0.5),
    }


decay_rate = 0.5
learn_rate = 0.01
clip_limit = 1.0
tiny_eps = 1e-30

def reference(tokens, weights, gradients, row_factors, col_factors):
    gradient = gradients.astype(jnp.float32)
    squares = gradient * gradient
    row_new = decay_rate * row_factors + (1.0 - decay_rate) * (lax.optimization_barrier(jnp.mean(squares, axis=2)) + tiny_eps)
    col_new = decay_rate * col_factors + (1.0 - decay_rate) * (lax.optimization_barrier(jnp.mean(squares, axis=1)) + tiny_eps)
    row_mean = lax.optimization_barrier(jnp.mean(row_new, axis=1))
    denominator = jnp.sqrt(row_new[:, :, None] * col_new[:, None, :] / row_mean[:, None, None])
    update = gradient / denominator
    rms_value = jnp.sqrt(lax.optimization_barrier(jnp.mean(update * update, axis=(1, 2))))
    clip_scale = jnp.maximum(1.0, rms_value / clip_limit)
    new_weights = (weights.astype(jnp.float32) - learn_rate * update / clip_scale[:, None, None]).astype(jnp.bfloat16)
    gate_proj = lax.dot_general(tokens, new_weights[0], (((1,), (1,)), ((), ())), preferred_element_type=jnp.float32)
    up_proj = lax.dot_general(tokens, new_weights[1], (((1,), (1,)), ((), ())), preferred_element_type=jnp.float32)
    hidden = (jax.nn.silu(gate_proj) * up_proj).astype(jnp.bfloat16)
    return (hidden, row_new, col_new)
```

```python
import jax
import jax.numpy as jnp
from jax import lax
from jax.experimental import pallas as pl
from jax.experimental.pallas import tpu as pltpu
from jax.sharding import Mesh
from jax.sharding import PartitionSpec as P

D = 8192
FF = 14336
AXES = ("yl", "x", "c", "yh", "z")
ROW = ("yl", "x", "c")
COL = ("yh", "z")
F32 = jnp.float32
BF16 = jnp.bfloat16
BY_MESH = pl.DeviceIdType.MESH

decay_rate = 0.5
learn_rate = 0.01
clip_limit = 1.0
tiny_eps = 1e-30

ROWS = 896
COLS = 1024
UNIT = 128
CHUNKS = ROWS // UNIT
LANES = 128
TILES = COLS // LANES
HALF = 1024
BLOCK = 256

COL_YL, ROW_YH, COL_C, ROW_Z, COL_X, SUM_C, SUM_X, SUM_Z, SUM_Y = 0, 1, 2, 3, 7, 11, 12, 16, 20
STAT_SEMS = 24


def spread(row):
    return jnp.transpose(jnp.broadcast_to(row, (LANES, LANES)))


def kernel(
    tok, wgt, grd, rowf, colf,
    out, row_out, col_out,
    g, w, wown, wpart, t, p, r, hid,
    colacc, colsrc, rowsrc, col_yl, row_yh, col_c, row_z, col_x,
    rn, cn, a, b, sumsrc, sum_c, sum_x, sum_z, sum_y,
    g_sem, w_sem, st_s, st_r, ty_s, ty_r, tx_s, tx_r, tc_s, tc_r, self_sem,
    wy_s, wy_r, rs_s, rs_r, out_sem,
):
    yl = lax.axis_index("yl")
    x = lax.axis_index("x")
    c = lax.axis_index("c")
    yh = lax.axis_index("yh")
    z = lax.axis_index("z")
    y = 2 * yh + yl

    def at_y(q):
        return {"yh": lax.div(q, 2), "yl": lax.rem(q, 2)}

    others = [1, 2, 3]
    x_of = [lax.rem(x + d, 4) for d in others]
    y_of = [lax.rem(y + d, 4) for d in others]
    z_of = [lax.rem(z + d, 4) for d in others]
    sibling = {"c": 1 - c}
    yl_peer = {"yl": 1 - yl}
    yh_peer = {"yh": 1 - yh}

    def remote(src, dst, s, q, device):
        return pltpu.make_async_remote_copy(
            src_ref=src, dst_ref=dst, send_sem=s, recv_sem=q,
            device_id=device, device_id_type=BY_MESH,
        )

    def g_copy(m, k):
        rows = pl.ds(k * UNIT, UNIT)
        return pltpu.make_async_copy(grd.at[m, rows], g.at[m, rows], g_sem.at[m, k])

    for m in range(2):
        for k in range(CHUNKS):
            g_copy(m, k).start()
    w_copies = [pltpu.make_async_copy(wgt.at[m], w.at[m], w_sem.at[m]) for m in range(2)]
    for copy in w_copies:
        copy.start()

    barrier = pltpu.get_barrier_semaphore()
    peers = [sibling]
    peers += [{"x": q} for q in x_of] + [at_y(q) for q in y_of] + [{"z": q} for q in z_of]
    for device in peers:
        pl.semaphore_signal(barrier, inc=1, device_id=device, device_id_type=BY_MESH)
    pl.semaphore_wait(barrier, len(peers))

    colacc[...] = jnp.zeros_like(colacc)
    rn[...] = jnp.ones_like(rn)
    rowsrc[...] = jnp.zeros_like(rowsrc)
    for m in range(2):
        def squares(k, carry):
            g_copy(m, k).wait()
            rows = pl.ds(pl.multiple_of(k * UNIT, UNIT), UNIT)
            total = jnp.zeros((UNIT, LANES), F32)
            for j in range(TILES):
                v = g[m, rows, j * LANES:(j + 1) * LANES].astype(F32)
                v = v * v
                total = total + v
                colacc[m * TILES + j] += jnp.sum(v.reshape(UNIT // 8, 8, LANES), axis=0)
            rowsrc[0, pl.ds(m * CHUNKS + k, 1), :] = jnp.sum(
                jnp.transpose(total), axis=0, keepdims=True
            )
            return carry

        lax.fori_loop(0, CHUNKS, squares, 0)
    colsrc[0] = jnp.sum(colacc[...], axis=1)

    to_yl = remote(colsrc.at[0], col_yl, st_s.at[COL_YL], st_r.at[COL_YL], yl_peer)
    to_yh = remote(rowsrc.at[0], row_yh, st_s.at[ROW_YH], st_r.at[ROW_YH], yh_peer)
    to_yl.start()
    to_yh.start()
    to_yl.wait_recv()
    colsrc[1] = colsrc[0] + col_yl[...]
    to_c = remote(colsrc.at[1], col_c, st_s.at[COL_C], st_r.at[COL_C], sibling)
    to_c.start()
    to_yh.wait_recv()
    rowsrc[1] = rowsrc[0] + row_yh[...]
    row_sends = []
    for q in z_of:
        copy = remote(rowsrc.at[1], row_z.at[z], st_s.at[ROW_Z + q], st_r.at[ROW_Z + z], {"z": q})
        copy.start()
        row_sends.append(copy)
    row_z[z] = rowsrc[1]

    home = (x * 2 + c) * 128
    mine = pl.ds(pl.multiple_of(home, 128), 128)

    def token_send(q):
        return remote(tok, t.at[yh, mine], ty_s.at[q], ty_r.at[yh], {"yh": yl, "yl": q})

    self_copy = pltpu.make_async_copy(tok, t.at[yh, mine], self_sem)
    for q in range(2):
        stays = (yl == q) & (yh == q)

        @pl.when(jnp.logical_not(stays))
        def _():
            token_send(q).start()

        @pl.when(stays)
        def _():
            self_copy.start()

    to_c.wait_recv()
    colsrc[2] = colsrc[1] + col_c[...]
    col_sends = []
    for q in x_of:
        copy = remote(colsrc.at[2], col_x.at[x], st_s.at[COL_X + q], st_r.at[COL_X + x], {"x": q})
        copy.start()
        col_sends.append(copy)
    col_x[x] = colsrc[2]

    for q in z_of:
        remote(rowsrc.at[1], row_z.at[q], st_s.at[ROW_Z + q], st_r.at[ROW_Z + q], {"z": q}).wait_recv()
    row_total = ((row_z[0] + row_z[1]) + row_z[2]) + row_z[3]
    for m in range(2):
        for k in range(CHUNKS):
            i = m * CHUNKS + k
            rn[i:i + 1] = decay_rate * rowf[m:m + 1, k * UNIT:(k + 1) * UNIT] + (1.0 - decay_rate) * (
                row_total[i:i + 1] / D + tiny_eps
            )
            row_out[m:m + 1, k * UNIT:(k + 1) * UNIT] = rn[i:i + 1]
    for q in x_of:
        remote(colsrc.at[2], col_x.at[q], st_s.at[COL_X + q], st_r.at[COL_X + q], {"x": q}).wait_recv()
    col_total = ((col_x[0] + col_x[1]) + col_x[2]) + col_x[3]
    for m in range(2):
        for j in range(TILES):
            i = m * TILES + j
            cn[i:i + 1] = decay_rate * colf[m:m + 1, j * LANES:(j + 1) * LANES] + (1.0 - decay_rate) * (
                col_total[i:i + 1] / FF + tiny_eps
            )
            col_out[m:m + 1, j * LANES:(j + 1) * LANES] = cn[i:i + 1]

    a[...] = 1.0 / rn[...]
    b[...] = 1.0 / cn[...]
    sumsrc[...] = jnp.zeros_like(sumsrc)
    for m in range(2):
        def norms(k, carry):
            rows = pl.ds(pl.multiple_of(k * UNIT, UNIT), UNIT)
            total = jnp.zeros((UNIT, LANES), F32)
            for j in range(TILES):
                v = g[m, rows, j * LANES:(j + 1) * LANES].astype(F32)
                total = total + v * v * b[m * TILES + j:m * TILES + j + 1]
            total = total * spread(a[pl.ds(m * CHUNKS + k, 1), :])
            return carry + jnp.sum(total.reshape(UNIT // 8, 8, LANES), axis=0)

        parts = lax.fori_loop(0, CHUNKS, norms, jnp.zeros((8, LANES), F32))
        sumsrc[0, m:m + 1] = jnp.sum(parts, axis=0, keepdims=True)
        sumsrc[0, 2 + m:3 + m] = jnp.sum(rn[m * CHUNKS:(m + 1) * CHUNKS], axis=0, keepdims=True)

    sum_sends = []
    to_c2 = remote(sumsrc.at[0], sum_c, st_s.at[SUM_C], st_r.at[SUM_C], sibling)
    to_c2.start()
    to_c2.wait_recv()
    sumsrc[1] = sumsrc[0] + sum_c[...]

    def exchange(src, dst, place, me, peers_of, device):
        for q in peers_of:
            copy = remote(src, dst.at[me], st_s.at[place + q], st_r.at[place + me], device(q))
            copy.start()
            sum_sends.append(copy)
        dst[me] = src[...]
        for q in peers_of:
            remote(src, dst.at[q], st_s.at[place + q], st_r.at[place + q], device(q)).wait_recv()
        return ((dst[0] + dst[1]) + dst[2]) + dst[3]

    sumsrc[2] = exchange(sumsrc.at[1], sum_x, SUM_X, x, x_of, lambda q: {"x": q})

    for q in range(2):
        stays = (yl == yh) & (yh == q)

        @pl.when(jnp.logical_not(stays))
        def _():
            remote(tok, t.at[q, mine], ty_s.at[q], ty_r.at[q], {"yh": yl, "yl": q}).wait_recv()

        @pl.when(stays)
        def _():
            self_copy.wait()

    def rows_of(q, core):
        return pl.ds(pl.multiple_of((q * 2 + core) * 128, 128), 128)

    def along_x(q, f, source):
        rows = rows_of(source, c)
        return remote(t.at[f, rows], t.at[f, rows], tx_s.at[q, f], tx_r.at[source, f], {"x": q})

    def to_sibling(q, f):
        rows = rows_of(q, c)
        return remote(t.at[f, rows], t.at[f, rows], tc_s.at[q, f], tc_r.at[q, f], sibling)

    for q in [x_of[0], x_of[2], x_of[1]]:
        for f in range(2):
            along_x(q, f, x).start()
    for f in range(2):
        to_sibling(x, f).start()

    sumsrc[3] = exchange(sumsrc.at[2], sum_z, SUM_Z, z, z_of, lambda q: {"z": q})
    total = exchange(sumsrc.at[3], sum_y, SUM_Y, y, y_of, at_y)

    for m in range(2):
        row_mean = jnp.sum(total[2 + m:3 + m], axis=1, keepdims=True) / (8.0 * FF)
        norm_total = jnp.sum(total[m:m + 1], axis=1, keepdims=True) * row_mean
        clip_scale = jnp.maximum(1.0, jnp.sqrt(norm_total / (FF * D)) / clip_limit)
        scale = learn_rate * jnp.sqrt(row_mean) / clip_scale
        a[m * CHUNKS:(m + 1) * CHUNKS] = scale / jnp.sqrt(rn[m * CHUNKS:(m + 1) * CHUNKS])
    b[...] = 1.0 / jnp.sqrt(cn[...])

    for copy in w_copies:
        copy.wait()

    def weight_send(k):
        return remote(wown.at[k], wpart.at[k], wy_s.at[k], wy_r.at[k], yh_peer)

    def update(k, carry):
        rows = pl.ds(pl.multiple_of(k * UNIT, UNIT), UNIT)
        for m in range(2):
            factor = spread(a[pl.ds(m * CHUNKS + k, 1), :])
            for j in range(TILES):
                cols = slice(j * LANES, (j + 1) * LANES)
                step = g[m, rows, cols].astype(F32) * factor * b[m * TILES + j:m * TILES + j + 1]
                wown[k, m * UNIT:(m + 1) * UNIT, cols] = (w[m, rows, cols].astype(F32) - step).astype(BF16)
        weight_send(k).start()
        return carry

    lax.fori_loop(0, CHUNKS, update, 0)

    for q in [x_of[0], x_of[2], x_of[1]]:
        for f in range(2):
            along_x(q, f, q).wait_recv()
            to_sibling(q, f).start()
    for q in [x] + [x_of[0], x_of[2], x_of[1]]:
        for f in range(2):
            rows = rows_of(q, 1 - c)
            remote(t.at[f, rows], t.at[f, rows], tc_s.at[q, f], tc_r.at[q, f], sibling).wait_recv()

    right = lax.rem(z + 1, 4)
    left = lax.rem(z + 3, 4)

    def block_of(side, s):
        return lax.rem(z + 3 - s, 4) if side == 0 else lax.rem(z + 1 + s, 4)

    def ring_copy(k, s, side):
        target = right if side == 0 else left
        return remote(
            p.at[k, block_of(side, s), side], r.at[k, s, side],
            rs_s.at[k, s, side], rs_r.at[k, s, side], {"z": target},
        )

    def times(i, k, half, weights):
        tokens = t[half, pl.ds(pl.multiple_of(i * BLOCK, BLOCK), BLOCK), :]
        return lax.dot_general(
            tokens, weights[k], (((1,), (1,)), ((), ())), preferred_element_type=F32
        )

    def own_products(k):
        def body(i, carry):
            v = times(i, k, yh, wown)
            p[k, i, 0] = v[:, :UNIT]
            p[k, i, 1] = v[:, UNIT:]
            return carry

        lax.fori_loop(0, 4, body, 0)

    def other_products(k):
        def body(i, carry):
            v = times(i, k, 1 - yh, wpart)
            p[k, i, 0] += v[:, :UNIT]
            p[k, i, 1] += v[:, UNIT:]
            return carry

        lax.fori_loop(0, 4, body, 0)

    def ring_step(k, s):
        for side in range(2):
            ring_copy(k, s - 1, side).wait_recv()
            p[k, block_of(side, s), side] += r[k, s - 1, side]
            ring_copy(k, s, side).start()

    def out_copy(k):
        return pltpu.make_async_copy(
            hid.at[k], out.at[:, pl.ds(pl.multiple_of(k * UNIT, UNIT), UNIT)], out_sem.at[k]
        )

    def finish(k):
        for side in range(2):
            ring_copy(k, 2, side).wait_recv()
        gate = p[k, z, 0] + r[k, 2, 0]
        up = p[k, z, 1] + r[k, 2, 1]
        hid[k] = (gate / (1.0 + jnp.exp(-gate)) * up).astype(BF16)
        out_copy(k).start()

    def work(i, carry):
        @pl.when(i < CHUNKS)
        def _():
            own_products(i)

        @pl.when((i >= 1) & (i < CHUNKS + 1))
        def _():
            ring_step(i - 1, 1)

        @pl.when((i >= 2) & (i < CHUNKS + 2))
        def _():
            ring_step(i - 2, 2)

        @pl.when(i >= 3)
        def _():
            finish(i - 3)

        @pl.when(i < CHUNKS)
        def _():
            weight_send(i).wait_recv()
            other_products(i)
            for side in range(2):
                ring_copy(i, 0, side).start()

        return carry

    lax.fori_loop(0, CHUNKS + 3, work, 0)

    to_yl.wait_send()
    to_yh.wait_send()
    to_c.wait_send()
    to_c2.wait_send()
    for copy in row_sends + col_sends + sum_sends:
        copy.wait_send()
    for q in range(2):
        @pl.when(jnp.logical_not((yl == q) & (yh == q)))
        def _():
            token_send(q).wait_send()
    for q in x_of:
        for f in range(2):
            along_x(q, f, x).wait_send()
    for q in range(4):
        for f in range(2):
            to_sibling(q, f).wait_send()

    def drain(k, carry):
        weight_send(k).wait_send()
        for s in range(3):
            for side in range(2):
                ring_copy(k, s, side).wait_send()
        out_copy(k).wait()
        return carry

    lax.fori_loop(0, CHUNKS, drain, 0)


def local(tokens, weights, gradients, row_factors, col_factors):
    vmem = pl.BlockSpec(memory_space=pltpu.VMEM)
    hbm = pl.BlockSpec(memory_space=pl.ANY)
    dma = pltpu.SemaphoreType.DMA
    scratch = [
        pltpu.VMEM((2, ROWS, COLS), BF16),
        pltpu.VMEM((2, ROWS, COLS), BF16),
        pltpu.VMEM((CHUNKS, 2 * UNIT, COLS), BF16),
        pltpu.VMEM((CHUNKS, 2 * UNIT, COLS), BF16),
        pltpu.VMEM((2, HALF, COLS), BF16),
        pltpu.VMEM((CHUNKS, 4, 2, BLOCK, UNIT), F32),
        pltpu.VMEM((CHUNKS, 3, 2, BLOCK, UNIT), F32),
        pltpu.VMEM((CHUNKS, BLOCK, UNIT), BF16),
        pltpu.VMEM((16, 8, LANES), F32),
        pltpu.VMEM((3, 16, LANES), F32),
        pltpu.VMEM((2, 16, LANES), F32),
        pltpu.VMEM((16, LANES), F32),
        pltpu.VMEM((16, LANES), F32),
        pltpu.VMEM((16, LANES), F32),
        pltpu.VMEM((4, 16, LANES), F32),
        pltpu.VMEM((4, 16, LANES), F32),
        pltpu.VMEM((16, LANES), F32),
        pltpu.VMEM((16, LANES), F32),
        pltpu.VMEM((16, LANES), F32),
        pltpu.VMEM((16, LANES), F32),
        pltpu.VMEM((4, 8, LANES), F32),
        pltpu.VMEM((8, LANES), F32),
        pltpu.VMEM((4, 8, LANES), F32),
        pltpu.VMEM((4, 8, LANES), F32),
        pltpu.VMEM((4, 8, LANES), F32),
        dma((2, CHUNKS)), dma((2,)), dma((STAT_SEMS,)), dma((STAT_SEMS,)),
        dma((2,)), dma((2,)), dma((4, 2)), dma((4, 2)), dma((4, 2)), dma((4, 2)), dma(()),
        dma((CHUNKS,)), dma((CHUNKS,)), dma((CHUNKS, 3, 2)), dma((CHUNKS, 3, 2)), dma((CHUNKS,)),
    ]
    return pl.pallas_call(
        kernel,
        out_shape=[
            jax.ShapeDtypeStruct((BLOCK, ROWS), BF16),
            jax.ShapeDtypeStruct((2, ROWS), F32),
            jax.ShapeDtypeStruct((2, COLS), F32),
        ],
        in_specs=[hbm, hbm, hbm, vmem, vmem],
        out_specs=[hbm, vmem, vmem],
        scratch_shapes=scratch,
        compiler_params=pltpu.CompilerParams(
            collective_id=0, has_side_effects=True, vmem_limit_bytes=60 * 2**20
        ),
        name="step",
    )(tokens, weights, gradients, row_factors, col_factors)


def solution(mesh):
    torus = Mesh(mesh.devices.reshape(2, 4, 2, 2, 4), AXES)
    in_specs = (P(ROW, COL), P(None, ROW, COL), P(None, ROW, COL), P(None, ROW), P(None, COL))
    out_specs = (P(COL, ROW), P(None, ROW), P(None, COL))
    return jax.shard_map(local, mesh=torus, in_specs=in_specs, out_specs=out_specs, check_vma=False)
```

```python
import jax
import jax.numpy as jnp
from jax import lax
from jax.experimental import pallas as pl
from jax.experimental.pallas import tpu as pltpu
from jax.sharding import Mesh
from jax.sharding import PartitionSpec as P

D = 8192
FF = 14336
AXES = ("yl", "x", "c", "yh", "z")
ROW = ("yl", "x", "c")
COL = ("yh", "z")
F32 = jnp.float32
BF16 = jnp.bfloat16
BY_MESH = pl.DeviceIdType.MESH

decay_rate = 0.5
learn_rate = 0.01
clip_limit = 1.0
tiny_eps = 1e-30

ROWS = 896
COLS = 1024
UNIT = 128
PAIRS = ROWS // UNIT
PIECE = 64
CHUNKS = ROWS // PIECE
LOCAL = 2
RINGS = CHUNKS + LOCAL
LAG = 2
LANES = 128
TILES = COLS // LANES
HALF = 1024
BLOCK = 256

COL_SUMS, ROW_SUMS, SUM_XC, SUM_YZ = 0, 16, 24, 32
STAT_SEMS = 48


def spread(row):
    return jnp.transpose(jnp.broadcast_to(row, (LANES, LANES)))


def kernel(
    tok, wgt, grd, rowf, colf,
    hid, row_out, col_out,
    g, w, wown, wpart, t, p, r, away, come, kept,
    colacc, colsrc, rowsrc, colin, rowin,
    rn, cn, a, b, sumsrc, sum_xc, sum_yz,
    g_sem, w_sem, st_s, st_r, ty_s, ty_r, tx_s, tx_r, tc_s, tc_r,
    wy_s, wy_r, rs_s, rs_r, fy_s, fy_r,
):
    yl = lax.axis_index("yl")
    x = lax.axis_index("x")
    c = lax.axis_index("c")
    yh = lax.axis_index("yh")
    z = lax.axis_index("z")
    y = 2 * yh + yl

    def at_row(q):
        return {"yl": lax.div(q, 8), "x": lax.rem(lax.div(q, 2), 4), "c": lax.rem(q, 2)}

    def at_col(q):
        return {"yh": lax.div(q, 4), "z": lax.rem(q, 4)}

    def at_xc(q):
        return {"x": lax.div(q, 2), "c": lax.rem(q, 2)}

    def at_yz(q):
        return {"yh": lax.div(q, 8), "yl": lax.rem(lax.div(q, 4), 2), "z": lax.rem(q, 4)}

    in_row = yl * 8 + x * 2 + c
    in_col = yh * 4 + z
    in_xc = x * 2 + c
    in_yz = y * 4 + z
    x_of = [lax.rem(x + d, 4) for d in (1, 3, 2)]
    sibling = {"c": 1 - c}
    yh_peer = {"yh": 1 - yh}

    def remote(src, dst, s, q, device):
        return pltpu.make_async_remote_copy(
            src_ref=src, dst_ref=dst, send_sem=s, recv_sem=q,
            device_id=device, device_id_type=BY_MESH,
        )

    def g_copy(m, k):
        rows = pl.ds(k * UNIT, UNIT)
        return pltpu.make_async_copy(grd.at[m, rows], g.at[m, rows], g_sem.at[m, k])

    for m in range(2):
        for k in range(PAIRS):
            g_copy(m, k).start()
    w_copies = [pltpu.make_async_copy(wgt.at[m], w.at[m], w_sem.at[m]) for m in range(2)]
    for copy in w_copies:
        copy.start()

    barrier = pltpu.get_barrier_semaphore()
    peers = [at_row(lax.rem(in_row + d, 16)) for d in range(1, 16)]
    peers += [at_yz(lax.rem(in_yz + d, 16)) for d in range(1, 16)]
    for device in peers:
        pl.semaphore_signal(barrier, inc=1, device_id=device, device_id_type=BY_MESH)
    colacc[...] = jnp.zeros_like(colacc)
    rn[...] = jnp.ones_like(rn)
    rowsrc[...] = jnp.zeros_like(rowsrc)
    for m in range(2):
        def squares(k, carry):
            g_copy(m, k).wait()
            rows = pl.ds(pl.multiple_of(k * UNIT, UNIT), UNIT)
            total = jnp.zeros((UNIT, LANES), F32)
            for j in range(TILES):
                v = g[m, rows, j * LANES:(j + 1) * LANES].astype(F32)
                v = v * v
                total = total + v
                colacc[m * TILES + j] += jnp.sum(v.reshape(UNIT // 8, 8, LANES), axis=0)
            rowsrc[pl.ds(m * PAIRS + k, 1), :] = jnp.sum(
                jnp.transpose(total), axis=0, keepdims=True
            )
            return carry

        lax.fori_loop(0, PAIRS, squares, 0)
    colsrc[...] = jnp.sum(colacc[...], axis=1)
    pl.semaphore_wait(barrier, len(peers))

    sent = []

    def give(src, slots, place, n, me, device_of):
        for d in range(1, n):
            q = lax.rem(me + d, n)
            copy = remote(src, slots.at[me], st_s.at[place + q], st_r.at[place + me], device_of(q))
            copy.start()
            sent.append(copy)
        slots[me] = src[...]

    def take(src, slots, place, n, me, device_of):
        for d in range(1, n):
            q = lax.rem(me + d, n)
            remote(src, slots.at[q], st_s.at[place + q], st_r.at[place + q], device_of(q)).wait_recv()
        total = slots[0]
        for q in range(1, n):
            total = total + slots[q]
        return total

    give(rowsrc, rowin, ROW_SUMS, 8, in_col, at_col)
    give(colsrc, colin, COL_SUMS, 16, in_row, at_row)

    def rows_of(q, core):
        return pl.ds(pl.multiple_of((q * 2 + core) * 128, 128), 128)

    mine = rows_of(x, c)
    same = yl == yh

    def token_send(q):
        return remote(tok, t.at[yh, mine], ty_s.at[q], ty_r.at[yh], {"yh": yl, "yl": q})

    other_send = remote(tok, t.at[2, mine], ty_s.at[2], ty_r.at[2], {"yl": 1 - yl})
    home = jnp.where(same, yh, 2)
    t[home, mine] = tok[...]
    early = [
        remote(tok, t.at[home, mine], tx_s.at[q, jnp.where(same, 0, 1)], tx_r.at[x, jnp.where(same, 0, 1)], {"x": q})
        for q in x_of[:2]
    ]
    for copy in early:
        copy.start()
    for q in range(2):
        @pl.when(jnp.logical_not(same & (yh == q)))
        def _():
            token_send(q).start()

    @pl.when(jnp.logical_not(same))
    def _():
        other_send.start()

    row_total = take(rowsrc, rowin, ROW_SUMS, 8, in_col, at_col)
    for m in range(2):
        for k in range(PAIRS):
            i = m * PAIRS + k
            rn[i:i + 1] = decay_rate * rowf[m:m + 1, k * UNIT:(k + 1) * UNIT] + (1.0 - decay_rate) * (
                row_total[i:i + 1] / D + tiny_eps
            )
            row_out[m:m + 1, k * UNIT:(k + 1) * UNIT] = rn[i:i + 1]
    col_total = take(colsrc, colin, COL_SUMS, 16, in_row, at_row)
    for m in range(2):
        for j in range(TILES):
            i = m * TILES + j
            cn[i:i + 1] = decay_rate * colf[m:m + 1, j * LANES:(j + 1) * LANES] + (1.0 - decay_rate) * (
                col_total[i:i + 1] / FF + tiny_eps
            )
            col_out[m:m + 1, j * LANES:(j + 1) * LANES] = cn[i:i + 1]

    a[...] = 1.0 / rn[...]
    b[...] = 1.0 / cn[...]
    sumsrc[...] = jnp.zeros_like(sumsrc)
    for m in range(2):
        def norms(k, carry):
            rows = pl.ds(pl.multiple_of(k * UNIT, UNIT), UNIT)
            total = jnp.zeros((UNIT, LANES), F32)
            for j in range(TILES):
                v = g[m, rows, j * LANES:(j + 1) * LANES].astype(F32)
                total = total + v * v * b[m * TILES + j:m * TILES + j + 1]
            total = total * spread(a[pl.ds(m * PAIRS + k, 1), :])
            return carry + jnp.sum(total.reshape(UNIT // 8, 8, LANES), axis=0)

        parts = lax.fori_loop(0, PAIRS, norms, jnp.zeros((8, LANES), F32))
        sumsrc[0, m:m + 1] = jnp.sum(parts, axis=0, keepdims=True)
        sumsrc[0, 2 + m:3 + m] = jnp.sum(rn[m * PAIRS:(m + 1) * PAIRS], axis=0, keepdims=True)

    give(sumsrc.at[0], sum_xc, SUM_XC, 8, in_xc, at_xc)
    sumsrc[1] = take(sumsrc.at[0], sum_xc, SUM_XC, 8, in_xc, at_xc)
    give(sumsrc.at[1], sum_yz, SUM_YZ, 16, in_yz, at_yz)

    slots = [yh, 2, 1 - yh]
    for f in range(2):
        @pl.when(jnp.logical_not(same & (yh == f)))
        def _():
            remote(tok, t.at[f, mine], ty_s.at[f], ty_r.at[f], yh_peer).wait_recv()

    @pl.when(same)
    def _():
        other_send.wait_recv()

    def along_x(q, f, source):
        rows = rows_of(source, c)
        slot = slots[f]
        return remote(t.at[slot, rows], t.at[slot, rows], tx_s.at[q, f], tx_r.at[source, f], {"x": q})

    def to_sibling(q, f):
        rows = rows_of(q, c)
        slot = slots[f]
        return remote(t.at[slot, rows], t.at[slot, rows], tc_s.at[q, f], tc_r.at[q, f], sibling)

    def from_sibling(q, f):
        rows = rows_of(q, 1 - c)
        slot = slots[f]
        return remote(t.at[slot, rows], t.at[slot, rows], tc_s.at[q, f], tc_r.at[q, f], sibling)

    for f in range(3):
        for q in x_of:
            if f < 2 and q is not x_of[2]:
                @pl.when(same if f == 1 else jnp.logical_not(same))
                def _():
                    along_x(q, f, x).start()
            else:
                along_x(q, f, x).start()
        to_sibling(x, f).start()

    total = take(sumsrc.at[1], sum_yz, SUM_YZ, 16, in_yz, at_yz)

    for m in range(2):
        row_mean = jnp.sum(total[2 + m:3 + m], axis=1, keepdims=True) / (8.0 * FF)
        norm_total = jnp.sum(total[m:m + 1], axis=1, keepdims=True) * row_mean
        clip_scale = jnp.maximum(1.0, jnp.sqrt(norm_total / (FF * D)) / clip_limit)
        scale = learn_rate * jnp.sqrt(row_mean) / clip_scale
        a[m * PAIRS:(m + 1) * PAIRS] = scale / jnp.sqrt(rn[m * PAIRS:(m + 1) * PAIRS])
    b[...] = 1.0 / jnp.sqrt(cn[...])

    for copy in w_copies:
        copy.wait()

    def weight_send(k):
        return remote(wown.at[k], wpart.at[k], wy_s.at[k], wy_r.at[k], yh_peer)

    def update(i, carry):
        k = lax.rem(i + LOCAL // 2, PAIRS)
        rows = pl.ds(pl.multiple_of(k * UNIT, UNIT), UNIT)
        for m in range(2):
            factor = spread(a[pl.ds(m * PAIRS + k, 1), :])
            for j in range(TILES):
                cols = slice(j * LANES, (j + 1) * LANES)
                step = g[m, rows, cols].astype(F32) * factor * b[m * TILES + j:m * TILES + j + 1]
                new = (w[m, rows, cols].astype(F32) - step).astype(BF16)
                for h in range(2):
                    wown[2 * k + h, m * PIECE:(m + 1) * PIECE, cols] = new[h * PIECE:(h + 1) * PIECE]
        for h in range(2):
            @pl.when(2 * k + h >= LOCAL)
            def _():
                weight_send(2 * k + h).start()

        return carry

    lax.fori_loop(0, PAIRS, update, 0)

    def gather_tokens(f):
        for q in x_of:
            along_x(q, f, q).wait_recv()
            to_sibling(q, f).start()
        for q in [x] + x_of:
            from_sibling(q, f).wait_recv()

    gather_tokens(0)
    gather_tokens(1)

    right = lax.rem(z + 1, 4)
    left = lax.rem(z + 3, 4)

    def block_of(side, s):
        return lax.rem(z + 3 - s, 4) if side == 0 else lax.rem(z + 1 + s, 4)

    def ring_copy(n, s, side):
        target = right if side == 0 else left
        return remote(
            p.at[n, block_of(side, s), side], r.at[n, s, side],
            rs_s.at[n, s, side], rs_r.at[n, s, side], {"z": target},
        )

    def times(i, slot, weights):
        tokens = t[slot, pl.ds(pl.multiple_of(i * 2 * BLOCK, 2 * BLOCK), 2 * BLOCK), :]
        v = lax.dot_general(
            tokens, weights[...], (((1,), (1,)), ((), ())), preferred_element_type=F32
        )
        return v.reshape(2, 2, BLOCK // 2, LANES)

    def own_products(n):
        k = jnp.where(n < LOCAL, n, n - LOCAL)
        slot = jnp.where(n < LOCAL, 2, yh)

        def body(i, carry):
            p[n, pl.ds(2 * i, 2)] = times(i, slot, wown.at[k])
            return carry

        lax.fori_loop(0, 2, body, 0)

    def other_products(n):
        def body(i, carry):
            p[n, pl.ds(2 * i, 2)] += times(i, 1 - yh, wpart.at[n - LOCAL])
            return carry

        lax.fori_loop(0, 2, body, 0)

    def ring_step(n, s):
        for side in range(2):
            ring_copy(n, s - 1, side).wait_recv()
            p[n, block_of(side, s), side] += r[n, s - 1, side]
            ring_copy(n, s, side).start()

    def hidden(k, v):
        v = v.reshape(BLOCK, LANES)
        gate = v[:, :PIECE]
        up = v[:, PIECE:]
        h = (gate / (1.0 + jnp.exp(-gate)) * up).astype(BF16)

        @pl.when(lax.rem(k, 2) == 0)
        def _():
            hid[lax.div(k, 2), :, :PIECE] = h

        @pl.when(lax.rem(k, 2) == 1)
        def _():
            hid[lax.div(k, 2), :, PIECE:] = h

    def final_send(n):
        return remote(away.at[n], come.at[n], fy_s.at[n], fy_r.at[n], yh_peer)

    def finish(n):
        for side in range(2):
            ring_copy(n, 2, side).wait_recv()
        v = p[n, z] + r[n, 2]

        @pl.when(n < LOCAL)
        def _():
            away[n] = v
            final_send(n).start()

        @pl.when((n >= LOCAL) & (n < 2 * LOCAL))
        def _():
            kept[n - LOCAL] = v

        @pl.when(n >= 2 * LOCAL)
        def _():
            hidden(n - LOCAL, v)

    def work(n, carry):
        @pl.when(n < RINGS)
        def _():
            own_products(n)

        for s in (1, 2):
            @pl.when((n >= s * LAG) & (n < RINGS + s * LAG))
            def _():
                ring_step(n - s * LAG, s)

        @pl.when(n >= 3 * LAG)
        def _():
            finish(n - 3 * LAG)

        @pl.when(n == 2 * LOCAL)
        def _():
            gather_tokens(2)

        @pl.when((n >= 2 * LOCAL) & (n < RINGS))
        def _():
            weight_send(n - LOCAL).wait_recv()
            other_products(n)

        @pl.when(n < RINGS)
        def _():
            for side in range(2):
                ring_copy(n, 0, side).start()

        return carry

    lax.fori_loop(0, RINGS + 3 * LAG, work, 0)

    def last(n, carry):
        final_send(n).wait_recv()
        hidden(n, kept[n] + come[n])
        return carry

    lax.fori_loop(0, LOCAL, last, 0)

    for copy in sent:
        copy.wait_send()
    for q in range(2):
        @pl.when(jnp.logical_not(same & (yh == q)))
        def _():
            token_send(q).wait_send()

    @pl.when(jnp.logical_not(same))
    def _():
        other_send.wait_send()

    for f in range(3):
        for q in x_of:
            along_x(q, f, x).wait_send()
        for q in range(4):
            to_sibling(q, f).wait_send()

    def drain(n, carry):
        @pl.when(n >= 2 * LOCAL)
        def _():
            weight_send(n - LOCAL).wait_send()

        @pl.when(n < LOCAL)
        def _():
            final_send(n).wait_send()

        for s in range(3):
            for side in range(2):
                ring_copy(n, s, side).wait_send()
        return carry

    lax.fori_loop(0, RINGS, drain, 0)


def writer(hid, row_new, col_new, hid_out, row_out, col_out, sem):
    copies = [
        pltpu.make_async_copy(hid.at[k], hid_out.at[:, k * UNIT:(k + 1) * UNIT], sem.at[k])
        for k in range(PAIRS)
    ]
    copies += [
        pltpu.make_async_copy(row_new, row_out, sem.at[PAIRS]),
        pltpu.make_async_copy(col_new, col_out, sem.at[PAIRS + 1]),
    ]
    for copy in copies:
        copy.start()
    for copy in copies:
        copy.wait()


def local(tokens, weights, gradients, row_factors, col_factors):
    vmem = pl.BlockSpec(memory_space=pltpu.VMEM)
    hbm = pl.BlockSpec(memory_space=pl.ANY)
    dma = pltpu.SemaphoreType.DMA
    scratch = [
        pltpu.VMEM((2, ROWS, COLS), BF16),
        pltpu.VMEM((2, ROWS, COLS), BF16),
        pltpu.VMEM((CHUNKS, 2 * PIECE, COLS), BF16),
        pltpu.VMEM((CHUNKS, 2 * PIECE, COLS), BF16),
        pltpu.VMEM((3, HALF, COLS), BF16),
        pltpu.VMEM((RINGS, 4, 2, BLOCK // 2, LANES), F32),
        pltpu.VMEM((RINGS, 3, 2, BLOCK // 2, LANES), F32),
        pltpu.VMEM((LOCAL, 2, BLOCK // 2, LANES), F32),
        pltpu.VMEM((LOCAL, 2, BLOCK // 2, LANES), F32),
        pltpu.VMEM((LOCAL, 2, BLOCK // 2, LANES), F32),
        pltpu.VMEM((16, 8, LANES), F32),
        pltpu.VMEM((16, LANES), F32),
        pltpu.VMEM((16, LANES), F32),
        pltpu.VMEM((16, 16, LANES), F32),
        pltpu.VMEM((8, 16, LANES), F32),
        pltpu.VMEM((16, LANES), F32),
        pltpu.VMEM((16, LANES), F32),
        pltpu.VMEM((16, LANES), F32),
        pltpu.VMEM((16, LANES), F32),
        pltpu.VMEM((2, 8, LANES), F32),
        pltpu.VMEM((8, 8, LANES), F32),
        pltpu.VMEM((16, 8, LANES), F32),
        dma((2, PAIRS)), dma((2,)), dma((STAT_SEMS,)), dma((STAT_SEMS,)),
        dma((3,)), dma((3,)), dma((4, 3)), dma((4, 3)), dma((4, 3)), dma((4, 3)),
        dma((CHUNKS,)), dma((CHUNKS,)), dma((RINGS, 3, 2)), dma((RINGS, 3, 2)),
        dma((LOCAL,)), dma((LOCAL,)),
    ]
    results = pl.pallas_call(
        kernel,
        out_shape=[
            pltpu.VMEM((PAIRS, BLOCK, UNIT), BF16),
            pltpu.VMEM((2, ROWS), F32),
            pltpu.VMEM((2, COLS), F32),
        ],
        in_specs=[vmem, hbm, hbm, vmem, vmem],
        out_specs=[vmem, vmem, vmem],
        scratch_shapes=scratch,
        compiler_params=pltpu.CompilerParams(
            collective_id=0, has_side_effects=True, vmem_limit_bytes=52 * 2**20
        ),
        name="step",
    )(tokens, weights, gradients, row_factors, col_factors)
    return pl.pallas_call(
        writer,
        out_shape=[
            jax.ShapeDtypeStruct((BLOCK, ROWS), BF16),
            jax.ShapeDtypeStruct((2, ROWS), F32),
            jax.ShapeDtypeStruct((2, COLS), F32),
        ],
        in_specs=[vmem, vmem, vmem],
        out_specs=[hbm, hbm, hbm],
        scratch_shapes=[dma((PAIRS + 2,))],
        compiler_params=pltpu.CompilerParams(vmem_limit_bytes=2**20),
        name="write",
    )(*results)


def solution(mesh):
    torus = Mesh(mesh.devices.reshape(2, 4, 2, 2, 4), AXES)
    in_specs = (P(ROW, COL), P(None, ROW, COL), P(None, ROW, COL), P(None, ROW), P(None, COL))
    out_specs = (P(COL, ROW), P(None, ROW), P(None, COL))
    return jax.shard_map(local, mesh=torus, in_specs=in_specs, out_specs=out_specs, check_vma=False)
```

```python
import jax
import jax.numpy as jnp
from jax import lax
from jax.experimental import pallas as pl
from jax.experimental.pallas import tpu as pltpu
from jax.sharding import Mesh
from jax.sharding import PartitionSpec as P

D = 8192
FF = 14336
AXES = ("yl", "x", "c", "yh", "z")
ROW = ("yl", "x", "c")
COL = ("yh", "z")
F32 = jnp.float32
BF16 = jnp.bfloat16
BY_MESH = pl.DeviceIdType.MESH

decay_rate = 0.5
learn_rate = 0.01
clip_limit = 1.0
tiny_eps = 1e-30

ROWS = 896
COLS = 1024
UNIT = 128
PAIRS = ROWS // UNIT
PIECE = 64
CHUNKS = ROWS // PIECE
LOCAL = 2
RINGS = CHUNKS + LOCAL
VMEM_LIMIT = 67043328 - 464 * 1024
LAG = 2
LANES = 128
TILES = COLS // LANES
HALF = 1024
BLOCK = 256

COL_SUMS, ROW_SUMS, SUM_XC, SUM_YZ = 0, 16, 24, 32
STAT_SEMS = 48


def spread(row):
    return jnp.transpose(jnp.broadcast_to(row, (LANES, LANES)))


def kernel(
    tok, wgt, grd, row_old, col_old,
    hid, row_out, col_out,
    rowf, colf, g, w, wown, wpart, t, p, r, away, come, kept,
    colacc, colsrc, rowsrc, colin, rowin,
    rn, cn, a, b, sumsrc, sum_xc, sum_yz,
    g_sem, w_sem, in_sem, st_s, st_r, ty_s, ty_r, nx_s, nx_r, fx_s, fx_r, tc_s, tc_r,
    wy_s, wy_r, rs_s, rs_r, fy_s, fy_r,
):
    yl = lax.axis_index("yl")
    x = lax.axis_index("x")
    c = lax.axis_index("c")
    yh = lax.axis_index("yh")
    z = lax.axis_index("z")
    y = 2 * yh + yl

    def at_row(q):
        return {"yl": lax.div(q, 8), "x": lax.rem(lax.div(q, 2), 4), "c": lax.rem(q, 2)}

    def at_col(q):
        return {"yh": lax.div(q, 4), "z": lax.rem(q, 4)}

    def at_xc(q):
        return {"x": lax.div(q, 2), "c": lax.rem(q, 2)}

    def at_yz(q):
        return {"yh": lax.div(q, 8), "yl": lax.rem(lax.div(q, 4), 2), "z": lax.rem(q, 4)}

    in_row = yl * 8 + x * 2 + c
    in_col = yh * 4 + z
    in_xc = x * 2 + c
    in_yz = y * 4 + z
    x_next = lax.rem(x + 1, 4)
    x_prev = lax.rem(x + 3, 4)
    x_far = lax.rem(x + 2, 4)
    sibling = {"c": 1 - c}
    yh_peer = {"yh": 1 - yh}

    def remote(src, dst, s, q, device):
        return pltpu.make_async_remote_copy(
            src_ref=src, dst_ref=dst, send_sem=s, recv_sem=q,
            device_id=device, device_id_type=BY_MESH,
        )

    def g_copy(m, k):
        rows = pl.ds(k * UNIT, UNIT)
        return pltpu.make_async_copy(grd.at[m, rows], g.at[m, rows], g_sem.at[m, k])

    for m in range(2):
        for k in range(PAIRS):
            g_copy(m, k).start()
    w_copies = [pltpu.make_async_copy(wgt.at[m], w.at[m], w_sem.at[m]) for m in range(2)]

    def rows_of(q, core):
        return pl.ds(pl.multiple_of((q * 2 + core) * 128, 128), 128)

    mine = rows_of(x, c)
    same = yl == yh
    slots = [jnp.where(same, yh, 2), jnp.where(same, 2, yh), 1 - yh]
    tok_copy = pltpu.make_async_copy(tok, t.at[slots[0], mine], in_sem.at[0])
    tok_copy.start()
    factor_copies = [
        pltpu.make_async_copy(row_old, rowf, in_sem.at[1]),
        pltpu.make_async_copy(col_old, colf, in_sem.at[2]),
    ]
    for copy in factor_copies + w_copies:
        copy.start()

    barrier = pltpu.get_barrier_semaphore()
    peers = [at_row(lax.rem(in_row + d, 16)) for d in range(1, 16)]
    peers += [at_yz(lax.rem(in_yz + d, 16)) for d in range(1, 16)]
    for device in peers:
        pl.semaphore_signal(barrier, inc=1, device_id=device, device_id_type=BY_MESH)
    colacc[...] = jnp.zeros_like(colacc)
    rn[...] = jnp.ones_like(rn)
    rowsrc[...] = jnp.zeros_like(rowsrc)
    for m in range(2):
        def squares(k, carry):
            g_copy(m, k).wait()
            rows = pl.ds(pl.multiple_of(k * UNIT, UNIT), UNIT)
            total = jnp.zeros((UNIT, LANES), F32)
            for j in range(TILES):
                v = g[m, rows, j * LANES:(j + 1) * LANES].astype(F32)
                v = v * v
                total = total + v
                colacc[m * TILES + j] += jnp.sum(v.reshape(UNIT // 8, 8, LANES), axis=0)
            rowsrc[pl.ds(m * PAIRS + k, 1), :] = jnp.sum(
                jnp.transpose(total), axis=0, keepdims=True
            )
            return carry

        lax.fori_loop(0, PAIRS, squares, 0)
    colsrc[...] = jnp.sum(colacc[...], axis=1)
    pl.semaphore_wait(barrier, len(peers))

    sent = []

    def give(src, slots, place, n, me, device_of):
        for d in range(1, n):
            q = lax.rem(me + d, n)
            copy = remote(src, slots.at[me], st_s.at[place + q], st_r.at[place + me], device_of(q))
            copy.start()
            sent.append(copy)
        slots[me] = src[...]

    def take(src, slots, place, n, me, device_of):
        for d in range(1, n):
            q = lax.rem(me + d, n)
            remote(src, slots.at[q], st_s.at[place + q], st_r.at[place + q], device_of(q)).wait_recv()
        total = slots[0]
        for q in range(1, n):
            total = total + slots[q]
        return total

    give(rowsrc, rowin, ROW_SUMS, 8, in_col, at_col)
    give(colsrc, colin, COL_SUMS, 16, in_row, at_row)

    def near(f, side):
        rows = mine
        return remote(
            t.at[slots[f], rows], t.at[slots[f], rows], nx_s.at[f, side], nx_r.at[f, side],
            {"x": x_next if side == 0 else x_prev},
        )

    def near_in(f, side):
        rows = rows_of(x_prev if side == 0 else x_next, c)
        return remote(
            t.at[slots[f], rows], t.at[slots[f], rows], nx_s.at[f, side], nx_r.at[f, side],
            {"x": x_next if side == 0 else x_prev},
        )

    def half_rows(q, side):
        return pl.ds(pl.multiple_of((q * 2 + c) * 128 + 64 * side, 64), 64)

    def onward(f, side):
        rows = half_rows(x_prev if side == 0 else x_next, side)
        return remote(
            t.at[slots[f], rows], t.at[slots[f], rows], fx_s.at[f, side], fx_r.at[f, side],
            {"x": x_next if side == 0 else x_prev},
        )

    def onward_in(f, side):
        rows = half_rows(x_far, side)
        return remote(
            t.at[slots[f], rows], t.at[slots[f], rows], fx_s.at[f, side], fx_r.at[f, side],
            {"x": x_next if side == 0 else x_prev},
        )

    def to_sibling(q, f):
        rows = rows_of(q, c)
        return remote(t.at[slots[f], rows], t.at[slots[f], rows], tc_s.at[q, f], tc_r.at[q, f], sibling)

    def from_sibling(q, f):
        rows = rows_of(q, 1 - c)
        return remote(t.at[slots[f], rows], t.at[slots[f], rows], tc_s.at[q, f], tc_r.at[q, f], sibling)

    pair_send = remote(t.at[slots[0], mine], t.at[slots[0], mine], ty_s.at[0], ty_r.at[0], {"yl": 1 - yl})
    pair_in = remote(t.at[slots[1], mine], t.at[slots[1], mine], ty_s.at[0], ty_r.at[0], {"yl": 1 - yl})
    across_send = remote(
        t.at[slots[0], mine], t.at[yh, mine], ty_s.at[1], ty_r.at[1], {"yl": 1 - yl, "yh": 1 - yh}
    )
    across_in = remote(
        t.at[slots[2], mine], t.at[slots[2], mine], ty_s.at[1], ty_r.at[1], {"yl": 1 - yl, "yh": 1 - yh}
    )
    far_send = remote(t.at[slots[0], mine], t.at[yh, mine], ty_s.at[2], ty_r.at[2], yh_peer)
    far_in = remote(t.at[slots[2], mine], t.at[slots[2], mine], ty_s.at[2], ty_r.at[2], yh_peer)

    def share(f):
        for side in range(2):
            near(f, side).start()
        to_sibling(x, f).start()

    def pass_on(f):
        for side in range(2):
            near_in(f, side).wait_recv()
            onward(f, side).start()
        to_sibling(x_prev, f).start()
        to_sibling(x_next, f).start()

    def complete(f):
        for side in range(2):
            onward_in(f, side).wait_recv()
        to_sibling(x_far, f).start()

    def complete_sibling(f):
        for q in (x, x_prev, x_next, x_far):
            from_sibling(q, f).wait_recv()

    tok_copy.wait()
    pair_send.start()
    share(0)
    for copy in factor_copies:
        copy.wait()

    row_total = take(rowsrc, rowin, ROW_SUMS, 8, in_col, at_col)
    for m in range(2):
        for k in range(PAIRS):
            i = m * PAIRS + k
            rn[i:i + 1] = decay_rate * rowf[m:m + 1, k * UNIT:(k + 1) * UNIT] + (1.0 - decay_rate) * (
                row_total[i:i + 1] / D + tiny_eps
            )
            row_out[m:m + 1, k * UNIT:(k + 1) * UNIT] = rn[i:i + 1]
    col_total = take(colsrc, colin, COL_SUMS, 16, in_row, at_row)
    for m in range(2):
        for j in range(TILES):
            i = m * TILES + j
            cn[i:i + 1] = decay_rate * colf[m:m + 1, j * LANES:(j + 1) * LANES] + (1.0 - decay_rate) * (
                col_total[i:i + 1] / FF + tiny_eps
            )
            col_out[m:m + 1, j * LANES:(j + 1) * LANES] = cn[i:i + 1]

    a[...] = 1.0 / rn[...]
    b[...] = 1.0 / cn[...]
    sumsrc[...] = jnp.zeros_like(sumsrc)
    for m in range(2):
        def norms(k, carry):
            rows = pl.ds(pl.multiple_of(k * UNIT, UNIT), UNIT)
            total = jnp.zeros((UNIT, LANES), F32)
            for j in range(TILES):
                v = g[m, rows, j * LANES:(j + 1) * LANES].astype(F32)
                total = total + v * v * b[m * TILES + j:m * TILES + j + 1]
            total = total * spread(a[pl.ds(m * PAIRS + k, 1), :])
            return carry + jnp.sum(total.reshape(UNIT // 8, 8, LANES), axis=0)

        parts = lax.fori_loop(0, PAIRS, norms, jnp.zeros((8, LANES), F32))
        sumsrc[0, m:m + 1] = jnp.sum(parts, axis=0, keepdims=True)
        sumsrc[0, 2 + m:3 + m] = jnp.sum(rn[m * PAIRS:(m + 1) * PAIRS], axis=0, keepdims=True)

    give(sumsrc.at[0], sum_yz, SUM_YZ, 16, in_yz, at_yz)

    @pl.when(jnp.logical_not(same))
    def _():
        across_send.start()
        far_send.start()

    pass_on(0)
    sumsrc[1] = take(sumsrc.at[0], sum_yz, SUM_YZ, 16, in_yz, at_yz)
    give(sumsrc.at[1], sum_xc, SUM_XC, 8, in_xc, at_xc)
    pair_in.wait_recv()
    share(1)
    total = take(sumsrc.at[1], sum_xc, SUM_XC, 8, in_xc, at_xc)

    for m in range(2):
        row_mean = jnp.sum(total[2 + m:3 + m], axis=1, keepdims=True) / (8.0 * FF)
        norm_total = jnp.sum(total[m:m + 1], axis=1, keepdims=True) * row_mean
        clip_scale = jnp.maximum(1.0, jnp.sqrt(norm_total / (FF * D)) / clip_limit)
        scale = learn_rate * jnp.sqrt(row_mean) / clip_scale
        a[m * PAIRS:(m + 1) * PAIRS] = scale / jnp.sqrt(rn[m * PAIRS:(m + 1) * PAIRS])
    b[...] = 1.0 / jnp.sqrt(cn[...])

    for copy in w_copies:
        copy.wait()

    def weight_send(k):
        return remote(wown.at[k], wpart.at[k], wy_s.at[k], wy_r.at[k], yh_peer)

    def update(i, carry):
        k = lax.rem(i + LOCAL // 2, PAIRS)
        rows = pl.ds(pl.multiple_of(k * UNIT, UNIT), UNIT)
        for m in range(2):
            factor = spread(a[pl.ds(m * PAIRS + k, 1), :])
            for j in range(TILES):
                cols = slice(j * LANES, (j + 1) * LANES)
                step = g[m, rows, cols].astype(F32) * factor * b[m * TILES + j:m * TILES + j + 1]
                new = (w[m, rows, cols].astype(F32) - step).astype(BF16)
                for h in range(2):
                    wown[2 * k + h, m * PIECE:(m + 1) * PIECE, cols] = new[h * PIECE:(h + 1) * PIECE]
        for h in range(2):
            @pl.when(2 * k + h >= LOCAL)
            def _():
                weight_send(2 * k + h).start()

        return carry

    lax.fori_loop(0, 3, update, 0)
    complete(0)

    @pl.when(jnp.logical_not(same))
    def _():
        across_in.wait_recv()
        share(2)

    lax.fori_loop(3, 5, update, 0)
    pass_on(1)
    lax.fori_loop(5, PAIRS, update, 0)
    complete(1)
    complete_sibling(0)
    complete_sibling(1)

    right = lax.rem(z + 1, 4)
    left = lax.rem(z + 3, 4)

    def block_of(side, s):
        return lax.rem(z + 3 - s, 4) if side == 0 else lax.rem(z + 1 + s, 4)

    def ring_copy(n, s, side):
        target = right if side == 0 else left
        return remote(
            p.at[n, block_of(side, s), side], r.at[n, s, side],
            rs_s.at[n, s, side], rs_r.at[n, s, side], {"z": target},
        )

    def times(block, slot, weights):
        tokens = t[slot, pl.ds(pl.multiple_of(block * BLOCK, BLOCK), BLOCK), :]
        v = lax.dot_general(
            tokens, weights[...], (((1,), (1,)), ((), ())), preferred_element_type=F32
        )
        return v.reshape(2, BLOCK // 2, LANES)

    def own_products(n):
        k = jnp.where(n < LOCAL, n, n - LOCAL)
        slot = jnp.where(n < LOCAL, 2, yh)
        for d in (3, 1, 2, 0):
            block = lax.rem(z + d, 4)
            p[n, block] = times(block, slot, wown.at[k])

    def other_products(n):
        for d in (3, 1, 2, 0):
            block = lax.rem(z + d, 4)
            p[n, block] += times(block, 1 - yh, wpart.at[n - LOCAL])
            if d in (3, 1):
                ring_copy(n, 0, 0 if d == 3 else 1).start()

    def ring_step(n, s):
        for side in range(2):
            ring_copy(n, s - 1, side).wait_recv()
            p[n, block_of(side, s), side] += r[n, s - 1, side]
            ring_copy(n, s, side).start()

    def hidden(k, v):
        v = v.reshape(BLOCK, LANES)
        gate = v[:, :PIECE]
        up = v[:, PIECE:]
        h = (gate / (1.0 + jnp.exp(-gate)) * up).astype(BF16)

        @pl.when(lax.rem(k, 2) == 0)
        def _():
            hid[lax.div(k, 2), :, :PIECE] = h

        @pl.when(lax.rem(k, 2) == 1)
        def _():
            hid[lax.div(k, 2), :, PIECE:] = h

    def final_send(n):
        return remote(away.at[n], come.at[n], fy_s.at[n], fy_r.at[n], yh_peer)

    def finish(n):
        for side in range(2):
            ring_copy(n, 2, side).wait_recv()
        v = p[n, z] + r[n, 2]

        @pl.when(n < LOCAL)
        def _():
            away[n] = v
            final_send(n).start()

        @pl.when((n >= LOCAL) & (n < 2 * LOCAL))
        def _():
            kept[n - LOCAL] = v

        @pl.when(n >= 2 * LOCAL)
        def _():
            hidden(n - LOCAL, v)

    def work(n, carry):
        @pl.when(n < RINGS)
        def _():
            own_products(n)

        for s in (1, 2):
            @pl.when((n >= s * LAG) & (n < RINGS + s * LAG))
            def _():
                ring_step(n - s * LAG, s)

        @pl.when(n >= 3 * LAG)
        def _():
            finish(n - 3 * LAG)

        @pl.when(n < 2 * LOCAL)
        def _():
            for side in range(2):
                ring_copy(n, 0, side).start()

        @pl.when(same & (n == 1))
        def _():
            far_in.wait_recv()
            share(2)

        @pl.when(n == 3)
        def _():
            pass_on(2)

        @pl.when(n == 2 * LOCAL)
        def _():
            complete(2)
            complete_sibling(2)

        @pl.when((n >= 2 * LOCAL) & (n < RINGS))
        def _():
            weight_send(n - LOCAL).wait_recv()
            other_products(n)

        return carry

    lax.fori_loop(0, RINGS + 3 * LAG, work, 0)

    def last(n, carry):
        final_send(n).wait_recv()
        hidden(n, kept[n] + come[n])
        return carry

    lax.fori_loop(0, LOCAL, last, 0)

    for copy in sent:
        copy.wait_send()
    pair_send.wait_send()

    @pl.when(jnp.logical_not(same))
    def _():
        across_send.wait_send()
        far_send.wait_send()

    for f in range(3):
        for side in range(2):
            near(f, side).wait_send()
            onward(f, side).wait_send()
        for q in range(4):
            to_sibling(q, f).wait_send()

    def drain(n, carry):
        @pl.when(n >= 2 * LOCAL)
        def _():
            weight_send(n - LOCAL).wait_send()

        @pl.when(n < LOCAL)
        def _():
            final_send(n).wait_send()

        for s in range(3):
            for side in range(2):
                ring_copy(n, s, side).wait_send()
        return carry

    lax.fori_loop(0, RINGS, drain, 0)


def writer(hid, row_new, col_new, hid_out, row_out, col_out, sem):
    copies = [
        pltpu.make_async_copy(hid.at[k], hid_out.at[:, k * UNIT:(k + 1) * UNIT], sem.at[k])
        for k in range(PAIRS)
    ]
    copies += [
        pltpu.make_async_copy(row_new, row_out, sem.at[PAIRS]),
        pltpu.make_async_copy(col_new, col_out, sem.at[PAIRS + 1]),
    ]
    for copy in copies:
        copy.start()
    for copy in copies:
        copy.wait()


def local(tokens, weights, gradients, row_factors, col_factors):
    vmem = pl.BlockSpec(memory_space=pltpu.VMEM)
    hbm = pl.BlockSpec(memory_space=pl.ANY)
    dma = pltpu.SemaphoreType.DMA
    scratch = [
        pltpu.VMEM((2, ROWS), F32),
        pltpu.VMEM((2, COLS), F32),
        pltpu.VMEM((2, ROWS, COLS), BF16),
        pltpu.VMEM((2, ROWS, COLS), BF16),
        pltpu.VMEM((CHUNKS, 2 * PIECE, COLS), BF16),
        pltpu.VMEM((CHUNKS, 2 * PIECE, COLS), BF16),
        pltpu.VMEM((3, HALF, COLS), BF16),
        pltpu.VMEM((RINGS, 4, 2, BLOCK // 2, LANES), F32),
        pltpu.VMEM((RINGS, 3, 2, BLOCK // 2, LANES), F32),
        pltpu.VMEM((LOCAL, 2, BLOCK // 2, LANES), F32),
        pltpu.VMEM((LOCAL, 2, BLOCK // 2, LANES), F32),
        pltpu.VMEM((LOCAL, 2, BLOCK // 2, LANES), F32),
        pltpu.VMEM((16, 8, LANES), F32),
        pltpu.VMEM((16, LANES), F32),
        pltpu.VMEM((16, LANES), F32),
        pltpu.VMEM((16, 16, LANES), F32),
        pltpu.VMEM((8, 16, LANES), F32),
        pltpu.VMEM((16, LANES), F32),
        pltpu.VMEM((16, LANES), F32),
        pltpu.VMEM((16, LANES), F32),
        pltpu.VMEM((16, LANES), F32),
        pltpu.VMEM((2, 8, LANES), F32),
        pltpu.VMEM((8, 8, LANES), F32),
        pltpu.VMEM((16, 8, LANES), F32),
        dma((2, PAIRS)), dma((2,)), dma((3,)), dma((STAT_SEMS,)), dma((STAT_SEMS,)),
        dma((3,)), dma((3,)), dma((3, 2)), dma((3, 2)), dma((3, 2)), dma((3, 2)), dma((4, 3)), dma((4, 3)),
        dma((CHUNKS,)), dma((CHUNKS,)), dma((RINGS, 3, 2)), dma((RINGS, 3, 2)),
        dma((LOCAL,)), dma((LOCAL,)),
    ]
    results = pl.pallas_call(
        kernel,
        out_shape=[
            pltpu.VMEM((PAIRS, BLOCK, UNIT), BF16),
            pltpu.VMEM((2, ROWS), F32),
            pltpu.VMEM((2, COLS), F32),
        ],
        in_specs=[hbm] * 5,
        out_specs=[vmem, vmem, vmem],
        scratch_shapes=scratch,
        compiler_params=pltpu.CompilerParams(
            collective_id=0, has_side_effects=True, vmem_limit_bytes=VMEM_LIMIT
        ),
        name="step",
    )(tokens, weights, gradients, row_factors, col_factors)
    return pl.pallas_call(
        writer,
        out_shape=[
            jax.ShapeDtypeStruct((BLOCK, ROWS), BF16),
            jax.ShapeDtypeStruct((2, ROWS), F32),
            jax.ShapeDtypeStruct((2, COLS), F32),
        ],
        in_specs=[vmem, vmem, vmem],
        out_specs=[hbm, hbm, hbm],
        scratch_shapes=[dma((PAIRS + 2,))],
        compiler_params=pltpu.CompilerParams(vmem_limit_bytes=2**20),
        name="write",
    )(*results)


def solution(mesh):
    torus = Mesh(mesh.devices.reshape(2, 4, 2, 2, 4), AXES)
    in_specs = (P(ROW, COL), P(None, ROW, COL), P(None, ROW, COL), P(None, ROW), P(None, COL))
    out_specs = (P(COL, ROW), P(None, ROW), P(None, COL))
    return jax.shard_map(local, mesh=torus, in_specs=in_specs, out_specs=out_specs, check_vma=False)
```

```python
import jax
import jax.numpy as jnp
from jax import lax
from jax.experimental import pallas as pl
from jax.experimental.pallas import tpu as pltpu
from jax.sharding import Mesh
from jax.sharding import PartitionSpec as P

D = 8192
FF = 14336
AXES = ("yl", "x", "c", "yh", "z")
ROW = ("yl", "x", "c")
COL = ("yh", "z")
F32 = jnp.float32
BF16 = jnp.bfloat16
BY_MESH = pl.DeviceIdType.MESH

decay_rate = 0.5
learn_rate = 0.01
clip_limit = 1.0
tiny_eps = 1e-30

ROWS = 896
COLS = 1024
UNIT = 128
PAIRS = ROWS // UNIT
CHUNKS = PAIRS
LOCAL = 4
RINGS = CHUNKS + LOCAL
VMEM_LIMIT = 67043328 - 464 * 1024
LAG = 2
WIDE = 2 * UNIT
VALUES = WIDE
MESSAGE = VALUES + 16
SPAN = 250.0
HALF_LOG = 125.0 * 0.6931471805599453
ORDER = [LOCAL, 0, LOCAL + 1] + list(range(1, LOCAL)) + list(range(LOCAL + 2, CHUNKS))
LANES = 128
TILES = COLS // LANES
HALF = 1024
BLOCK = 256

COL_SUMS, ROW_SUMS, SUM_XC, SUM_YZ = 0, 16, 24, 32
STAT_SEMS = 48


def spread(row):
    return jnp.transpose(jnp.broadcast_to(row, (LANES, LANES)))


def put_code(ref, v):
    v = v.reshape(-1, 8, LANES)
    top = jnp.maximum(jnp.max(jnp.abs(v), axis=0) * 1.004, 1e-30).astype(BF16)
    factor = SPAN / top.astype(F32)
    q = jnp.exp2(jnp.abs(v) * factor - SPAN / 2.0)
    ref[:VALUES] = jnp.where(v < 0.0, -q, q).reshape(VALUES, LANES).astype(BF16)
    ref[VALUES:] = jnp.concatenate([top, top], axis=0)


def get_code(ref):
    top = ref[VALUES:].astype(F32)[:8]
    q = ref[:VALUES].astype(F32).reshape(-1, 8, LANES)
    v = (jnp.log(jnp.abs(q)) + HALF_LOG) * (top * (1.0 / (2.0 * HALF_LOG)))
    return jnp.where(q < 0.0, -v, v).reshape(VALUES, LANES)


def kernel(
    tok, wgt, grd, row_old, col_old,
    hid, row_out, col_out,
    rowf, colf, g, w, wown, wpart, t, p, e, r, away, come, kept,
    colacc, colsrc, rowsrc, colin, rowin,
    rn, cn, a, b, sumsrc, sum_xc, sum_yz,
    g_sem, w_sem, in_sem, st_s, st_r, ty_s, ty_r, nx_s, nx_r, fx_s, fx_r, tc_s, tc_r,
    wy_s, wy_r, rs_s, rs_r, fy_s, fy_r,
):
    yl = lax.axis_index("yl")
    x = lax.axis_index("x")
    c = lax.axis_index("c")
    yh = lax.axis_index("yh")
    z = lax.axis_index("z")
    y = 2 * yh + yl

    def at_row(q):
        return {"yl": lax.div(q, 8), "x": lax.rem(lax.div(q, 2), 4), "c": lax.rem(q, 2)}

    def at_col(q):
        return {"yh": lax.div(q, 4), "z": lax.rem(q, 4)}

    def at_xc(q):
        return {"x": lax.div(q, 2), "c": lax.rem(q, 2)}

    def at_yz(q):
        return {"yh": lax.div(q, 8), "yl": lax.rem(lax.div(q, 4), 2), "z": lax.rem(q, 4)}

    in_row = yl * 8 + x * 2 + c
    in_col = yh * 4 + z
    in_xc = x * 2 + c
    in_yz = y * 4 + z
    x_next = lax.rem(x + 1, 4)
    x_prev = lax.rem(x + 3, 4)
    x_far = lax.rem(x + 2, 4)
    sibling = {"c": 1 - c}
    yh_peer = {"yh": 1 - yh}

    def remote(src, dst, s, q, device):
        return pltpu.make_async_remote_copy(
            src_ref=src, dst_ref=dst, send_sem=s, recv_sem=q,
            device_id=device, device_id_type=BY_MESH,
        )

    def g_copy(m, k):
        rows = pl.ds(k * UNIT, UNIT)
        return pltpu.make_async_copy(grd.at[m, rows], g.at[m, rows], g_sem.at[m, k])

    for m in range(2):
        for k in range(PAIRS):
            g_copy(m, k).start()
    w_copies = [pltpu.make_async_copy(wgt.at[m], w.at[m], w_sem.at[m]) for m in range(2)]

    def rows_of(q, core):
        return pl.ds(pl.multiple_of((q * 2 + core) * 128, 128), 128)

    mine = rows_of(x, c)
    same = yl == yh
    slots = [jnp.where(same, yh, 2), jnp.where(same, 2, yh), 1 - yh]
    tok_copy = pltpu.make_async_copy(tok, t.at[slots[0], mine], in_sem.at[0])
    tok_copy.start()
    factor_copies = [
        pltpu.make_async_copy(row_old, rowf, in_sem.at[1]),
        pltpu.make_async_copy(col_old, colf, in_sem.at[2]),
    ]
    for copy in factor_copies + w_copies:
        copy.start()

    barrier = pltpu.get_barrier_semaphore()
    peers = [at_row(lax.rem(in_row + d, 16)) for d in range(1, 16)]
    peers += [at_yz(lax.rem(in_yz + d, 16)) for d in range(1, 16)]
    for device in peers:
        pl.semaphore_signal(barrier, inc=1, device_id=device, device_id_type=BY_MESH)
    colacc[...] = jnp.zeros_like(colacc)
    rn[...] = jnp.ones_like(rn)
    rowsrc[...] = jnp.zeros_like(rowsrc)
    for m in range(2):
        def squares(k, carry):
            g_copy(m, k).wait()
            rows = pl.ds(pl.multiple_of(k * UNIT, UNIT), UNIT)
            total = jnp.zeros((UNIT, LANES), F32)
            for j in range(TILES):
                v = g[m, rows, j * LANES:(j + 1) * LANES].astype(F32)
                v = v * v
                total = total + v
                colacc[m * TILES + j] += jnp.sum(v.reshape(UNIT // 8, 8, LANES), axis=0)
            rowsrc[pl.ds(m * PAIRS + k, 1), :] = jnp.sum(
                jnp.transpose(total), axis=0, keepdims=True
            )
            return carry

        lax.fori_loop(0, PAIRS, squares, 0)
    colsrc[...] = jnp.sum(colacc[...], axis=1)
    pl.semaphore_wait(barrier, len(peers))

    sent = []

    def give(src, slots, place, n, me, device_of):
        for d in range(1, n):
            q = lax.rem(me + d, n)
            copy = remote(src, slots.at[me], st_s.at[place + q], st_r.at[place + me], device_of(q))
            copy.start()
            sent.append(copy)
        slots[me] = src[...]

    def arrive(src, slots, place, n, me, device_of):
        for d in range(1, n):
            q = lax.rem(me + d, n)
            remote(src, slots.at[q], st_s.at[place + q], st_r.at[place + q], device_of(q)).wait_recv()

    def take(src, slots, place, n, me, device_of):
        arrive(src, slots, place, n, me, device_of)
        total = slots[0]
        for q in range(1, n):
            total = total + slots[q]
        return total

    give(rowsrc, rowin, ROW_SUMS, 8, in_col, at_col)
    give(colsrc, colin, COL_SUMS, 16, in_row, at_row)

    def near(f, side):
        rows = mine
        return remote(
            t.at[slots[f], rows], t.at[slots[f], rows], nx_s.at[f, side], nx_r.at[f, side],
            {"x": x_next if side == 0 else x_prev},
        )

    def near_in(f, side):
        rows = rows_of(x_prev if side == 0 else x_next, c)
        return remote(
            t.at[slots[f], rows], t.at[slots[f], rows], nx_s.at[f, side], nx_r.at[f, side],
            {"x": x_next if side == 0 else x_prev},
        )

    def half_rows(q, side):
        return pl.ds(pl.multiple_of((q * 2 + c) * 128 + 64 * side, 64), 64)

    def onward(f, side):
        rows = half_rows(x_prev if side == 0 else x_next, side)
        return remote(
            t.at[slots[f], rows], t.at[slots[f], rows], fx_s.at[f, side], fx_r.at[f, side],
            {"x": x_next if side == 0 else x_prev},
        )

    def onward_in(f, side):
        rows = half_rows(x_far, side)
        return remote(
            t.at[slots[f], rows], t.at[slots[f], rows], fx_s.at[f, side], fx_r.at[f, side],
            {"x": x_next if side == 0 else x_prev},
        )

    def to_sibling(q, f):
        rows = rows_of(q, c)
        return remote(t.at[slots[f], rows], t.at[slots[f], rows], tc_s.at[q, f], tc_r.at[q, f], sibling)

    def from_sibling(q, f):
        rows = rows_of(q, 1 - c)
        return remote(t.at[slots[f], rows], t.at[slots[f], rows], tc_s.at[q, f], tc_r.at[q, f], sibling)

    pair_send = remote(t.at[slots[0], mine], t.at[slots[0], mine], ty_s.at[0], ty_r.at[0], {"yl": 1 - yl})
    pair_in = remote(t.at[slots[1], mine], t.at[slots[1], mine], ty_s.at[0], ty_r.at[0], {"yl": 1 - yl})
    across_send = remote(
        t.at[slots[0], mine], t.at[yh, mine], ty_s.at[1], ty_r.at[1], {"yl": 1 - yl, "yh": 1 - yh}
    )
    across_in = remote(
        t.at[slots[2], mine], t.at[slots[2], mine], ty_s.at[1], ty_r.at[1], {"yl": 1 - yl, "yh": 1 - yh}
    )
    far_send = remote(t.at[slots[0], mine], t.at[yh, mine], ty_s.at[2], ty_r.at[2], yh_peer)
    far_in = remote(t.at[slots[2], mine], t.at[slots[2], mine], ty_s.at[2], ty_r.at[2], yh_peer)

    def share(f):
        for side in range(2):
            near(f, side).start()
        to_sibling(x, f).start()

    def pass_on(f):
        for side in range(2):
            near_in(f, side).wait_recv()
            onward(f, side).start()
        to_sibling(x_prev, f).start()
        to_sibling(x_next, f).start()

    def complete(f):
        for side in range(2):
            onward_in(f, side).wait_recv()
        to_sibling(x_far, f).start()

    def complete_sibling(f):
        for q in (x, x_prev, x_next, x_far):
            from_sibling(q, f).wait_recv()

    tok_copy.wait()
    pair_send.start()

    @pl.when(jnp.logical_not(same))
    def _():
        across_send.start()
        far_send.start()

    share(0)
    for copy in factor_copies:
        copy.wait()

    for copy in w_copies:
        copy.wait()
    sumsrc[...] = jnp.zeros_like(sumsrc)

    row_total = take(rowsrc, rowin, ROW_SUMS, 8, in_col, at_col)
    for m in range(2):
        for k in range(PAIRS):
            i = m * PAIRS + k
            rn[i:i + 1] = decay_rate * rowf[m:m + 1, k * UNIT:(k + 1) * UNIT] + (1.0 - decay_rate) * (
                row_total[i:i + 1] / D + tiny_eps
            )
            row_out[m:m + 1, k * UNIT:(k + 1) * UNIT] = rn[i:i + 1]
    col_total = take(colsrc, colin, COL_SUMS, 16, in_row, at_row)
    for m in range(2):
        for j in range(TILES):
            i = m * TILES + j
            cn[i:i + 1] = decay_rate * colf[m:m + 1, j * LANES:(j + 1) * LANES] + (1.0 - decay_rate) * (
                col_total[i:i + 1] / FF + tiny_eps
            )
            col_out[m:m + 1, j * LANES:(j + 1) * LANES] = cn[i:i + 1]

    a[...] = 1.0 / rn[...]
    b[...] = 1.0 / cn[...]
    for m in range(2):
        def norms(k, carry):
            rows = pl.ds(pl.multiple_of(k * UNIT, UNIT), UNIT)
            total = jnp.zeros((UNIT, LANES), F32)
            for j in range(TILES):
                v = g[m, rows, j * LANES:(j + 1) * LANES].astype(F32)
                total = total + v * v * b[m * TILES + j:m * TILES + j + 1]
            total = total * spread(a[pl.ds(m * PAIRS + k, 1), :])
            return carry + jnp.sum(total.reshape(UNIT // 8, 8, LANES), axis=0)

        parts = lax.fori_loop(0, PAIRS, norms, jnp.zeros((8, LANES), F32))
        sumsrc[0, m:m + 1] = jnp.sum(parts, axis=0, keepdims=True)
        sumsrc[0, 2 + m:3 + m] = jnp.sum(rn[m * PAIRS:(m + 1) * PAIRS], axis=0, keepdims=True)

    give(sumsrc.at[0], sum_xc, SUM_XC, 8, in_xc, at_xc)
    pair_in.wait_recv()
    share(1)
    pass_on(0)
    sumsrc[1] = take(sumsrc.at[0], sum_xc, SUM_XC, 8, in_xc, at_xc)
    give(sumsrc.at[1], sum_yz, SUM_YZ, 16, in_yz, at_yz)
    total = take(sumsrc.at[1], sum_yz, SUM_YZ, 16, in_yz, at_yz)

    for m in range(2):
        row_mean = jnp.sum(total[2 + m:3 + m], axis=1, keepdims=True) / (8.0 * FF)
        norm_total = jnp.sum(total[m:m + 1], axis=1, keepdims=True) * row_mean
        clip_scale = jnp.maximum(1.0, jnp.sqrt(norm_total / (FF * D)) / clip_limit)
        scale = learn_rate * jnp.sqrt(row_mean) / clip_scale
        a[m * PAIRS:(m + 1) * PAIRS] = scale / jnp.sqrt(rn[m * PAIRS:(m + 1) * PAIRS])
    b[...] = 1.0 / jnp.sqrt(cn[...])

    def weight_send(k):
        return remote(wown.at[k], wpart.at[k - LOCAL], wy_s.at[k], wy_r.at[k], yh_peer)

    def update(i, carry):
        k = ORDER[-1]
        for q in range(CHUNKS - 1):
            k = jnp.where(i == q, ORDER[q], k)
        rows = pl.ds(pl.multiple_of(k * UNIT, UNIT), UNIT)
        for m in range(2):
            factor = spread(a[pl.ds(m * PAIRS + k, 1), :])
            for j in range(TILES):
                cols = slice(j * LANES, (j + 1) * LANES)
                step = g[m, rows, cols].astype(F32) * factor * b[m * TILES + j:m * TILES + j + 1]
                wown[k, m * UNIT:(m + 1) * UNIT, cols] = (w[m, rows, cols].astype(F32) - step).astype(BF16)

        @pl.when(k >= LOCAL)
        def _():
            weight_send(k).start()

        return carry

    lax.fori_loop(0, 1, update, 0)
    pass_on(1)

    @pl.when(same)
    def _():
        far_in.wait_recv()

    @pl.when(jnp.logical_not(same))
    def _():
        across_in.wait_recv()

    share(2)
    lax.fori_loop(1, 3, update, 0)
    complete(0)
    complete(1)
    complete_sibling(0)
    complete_sibling(1)

    right = lax.rem(z + 1, 4)
    left = lax.rem(z + 3, 4)

    def block_of(side, s):
        return lax.rem(z + 3 - s, 4) if side == 0 else lax.rem(z + 1 + s, 4)

    def ring_copy(n, s, side):
        target = right if side == 0 else left
        return remote(
            e.at[n, s, side], r.at[n, s, side],
            rs_s.at[n, s, side], rs_r.at[n, s, side], {"z": target},
        )

    def times(block, slot, weights):
        tokens = t[slot, pl.ds(pl.multiple_of(block * BLOCK, BLOCK), BLOCK), :]
        return lax.dot_general(
            tokens, weights[...], (((1,), (1,)), ((), ())), preferred_element_type=F32
        )

    def arrange(v):
        parts = []
        for side in range(2):
            rows = slice(side * (BLOCK // 2), (side + 1) * (BLOCK // 2))
            parts.append(jnp.concatenate([v[rows, :UNIT], v[rows, UNIT:]], axis=0))
        return parts

    def begin(n, d, parts):
        if d in (3, 1):
            side = 0 if d == 3 else 1
            put_code(e.at[n, 0, side], parts[side])
            ring_copy(n, 0, side).start()

    def local_products(n):
        k = jnp.where(n < LOCAL, n, n - LOCAL)
        slot = jnp.where(n < LOCAL, 2, yh)
        for d in (3, 1, 2, 0):
            block = lax.rem(z + d, 4)
            parts = arrange(times(block, slot, wown.at[k]))
            for side in range(2):
                p[n, block, side] = parts[side]
            begin(n, d, parts)

    def own_products(n):
        for d in (3, 1, 2, 0):
            block = lax.rem(z + d, 4)
            parts = arrange(times(block, yh, wown.at[n - LOCAL]))
            for side in range(2):
                p[n, block, side] = parts[side]

    def other_products(n):
        for d in (3, 1, 2, 0):
            block = lax.rem(z + d, 4)
            parts = arrange(times(block, 1 - yh, wpart.at[n - 2 * LOCAL]))
            for side in range(2):
                parts[side] = parts[side] + p[n, block, side]
                p[n, block, side] = parts[side]
            begin(n, d, parts)

    def ring_step(n, s):
        for side in range(2):
            ring_copy(n, s - 1, side).wait_recv()
            put_code(e.at[n, s, side], p[n, block_of(side, s), side] + get_code(r.at[n, s - 1, side]))
            ring_copy(n, s, side).start()

    def hidden(k, side, v):
        gate = v[:UNIT]
        up = v[UNIT:]
        rows = slice(side * (BLOCK // 2), (side + 1) * (BLOCK // 2))
        hid[k, rows] = (gate / (1.0 + jnp.exp(-gate)) * up).astype(BF16)

    def final_send(n):
        return remote(away.at[n], come.at[n], fy_s.at[n], fy_r.at[n], yh_peer)

    def finish(n):
        for side in range(2):
            ring_copy(n, 2, side).wait_recv()
            v = p[n, z, side] + get_code(r.at[n, 2, side])

            @pl.when(n < LOCAL)
            def _():
                put_code(away.at[n, side], v)

            @pl.when((n >= LOCAL) & (n < 2 * LOCAL))
            def _():
                kept[n - LOCAL, side] = v

            @pl.when(n >= 2 * LOCAL)
            def _():
                hidden(n - LOCAL, side, v)

        @pl.when(n < LOCAL)
        def _():
            final_send(n).start()

    def work(n, carry):
        @pl.when(n < 2 * LOCAL)
        def _():
            local_products(n)

        @pl.when((n >= 2 * LOCAL) & (n < RINGS))
        def _():
            own_products(n)

        @pl.when(n < PAIRS - 3)
        def _():
            update(n + 3, 0)

        for s in (1, 2):
            @pl.when((n >= s * LAG) & (n < RINGS + s * LAG))
            def _():
                ring_step(n - s * LAG, s)

        @pl.when(n >= 3 * LAG)
        def _():
            finish(n - 3 * LAG)

        @pl.when(n == 2)
        def _():
            pass_on(2)

        @pl.when(n == 2 * LOCAL)
        def _():
            complete(2)
            complete_sibling(2)

        @pl.when((n >= 2 * LOCAL) & (n < RINGS))
        def _():
            weight_send(n - LOCAL).wait_recv()
            other_products(n)

        return carry

    lax.fori_loop(0, RINGS + 3 * LAG, work, 0)

    def last(n, carry):
        final_send(n).wait_recv()
        for side in range(2):
            hidden(n, side, kept[n, side] + get_code(come.at[n, side]))
        return carry

    lax.fori_loop(0, LOCAL, last, 0)

    for copy in sent:
        copy.wait_send()
    pair_send.wait_send()

    @pl.when(jnp.logical_not(same))
    def _():
        across_send.wait_send()
        far_send.wait_send()

    for f in range(3):
        for side in range(2):
            near(f, side).wait_send()
            onward(f, side).wait_send()
        for q in range(4):
            to_sibling(q, f).wait_send()

    def drain(n, carry):
        @pl.when(n >= 2 * LOCAL)
        def _():
            weight_send(n - LOCAL).wait_send()

        @pl.when(n < LOCAL)
        def _():
            final_send(n).wait_send()

        for s in range(3):
            for side in range(2):
                ring_copy(n, s, side).wait_send()
        return carry

    lax.fori_loop(0, RINGS, drain, 0)


def writer(hid, row_new, col_new, hid_out, row_out, col_out, sem):
    copies = [
        pltpu.make_async_copy(hid.at[k], hid_out.at[:, k * UNIT:(k + 1) * UNIT], sem.at[k])
        for k in range(PAIRS)
    ]
    copies += [
        pltpu.make_async_copy(row_new, row_out, sem.at[PAIRS]),
        pltpu.make_async_copy(col_new, col_out, sem.at[PAIRS + 1]),
    ]
    for copy in copies:
        copy.start()
    for copy in copies:
        copy.wait()


def local(tokens, weights, gradients, row_factors, col_factors):
    vmem = pl.BlockSpec(memory_space=pltpu.VMEM)
    hbm = pl.BlockSpec(memory_space=pl.ANY)
    dma = pltpu.SemaphoreType.DMA
    scratch = [
        pltpu.VMEM((2, ROWS), F32),
        pltpu.VMEM((2, COLS), F32),
        pltpu.VMEM((2, ROWS, COLS), BF16),
        pltpu.VMEM((2, ROWS, COLS), BF16),
        pltpu.VMEM((CHUNKS, WIDE, COLS), BF16),
        pltpu.VMEM((CHUNKS - LOCAL, WIDE, COLS), BF16),
        pltpu.VMEM((3, HALF, COLS), BF16),
        pltpu.VMEM((RINGS, 4, 2, VALUES, LANES), F32),
        pltpu.VMEM((RINGS, 3, 2, MESSAGE, LANES), BF16),
        pltpu.VMEM((RINGS, 3, 2, MESSAGE, LANES), BF16),
        pltpu.VMEM((LOCAL, 2, MESSAGE, LANES), BF16),
        pltpu.VMEM((LOCAL, 2, MESSAGE, LANES), BF16),
        pltpu.VMEM((LOCAL, 2, VALUES, LANES), F32),
        pltpu.VMEM((16, 8, LANES), F32),
        pltpu.VMEM((16, LANES), F32),
        pltpu.VMEM((16, LANES), F32),
        pltpu.VMEM((16, 16, LANES), F32),
        pltpu.VMEM((8, 16, LANES), F32),
        pltpu.VMEM((16, LANES), F32),
        pltpu.VMEM((16, LANES), F32),
        pltpu.VMEM((16, LANES), F32),
        pltpu.VMEM((16, LANES), F32),
        pltpu.VMEM((2, 8, LANES), F32),
        pltpu.VMEM((8, 8, LANES), F32),
        pltpu.VMEM((16, 8, LANES), F32),
        dma((2, PAIRS)), dma((2,)), dma((3,)), dma((STAT_SEMS,)), dma((STAT_SEMS,)),
        dma((3,)), dma((3,)), dma((3, 2)), dma((3, 2)), dma((3, 2)), dma((3, 2)), dma((4, 3)), dma((4, 3)),
        dma((CHUNKS,)), dma((CHUNKS,)), dma((RINGS, 3, 2)), dma((RINGS, 3, 2)),
        dma((LOCAL,)), dma((LOCAL,)),
    ]
    results = pl.pallas_call(
        kernel,
        out_shape=[
            pltpu.VMEM((PAIRS, BLOCK, UNIT), BF16),
            pltpu.VMEM((2, ROWS), F32),
            pltpu.VMEM((2, COLS), F32),
        ],
        in_specs=[hbm] * 5,
        out_specs=[vmem, vmem, vmem],
        scratch_shapes=scratch,
        compiler_params=pltpu.CompilerParams(
            collective_id=0, has_side_effects=True, vmem_limit_bytes=VMEM_LIMIT
        ),
        name="step",
    )(tokens, weights, gradients, row_factors, col_factors)
    return pl.pallas_call(
        writer,
        out_shape=[
            jax.ShapeDtypeStruct((BLOCK, ROWS), BF16),
            jax.ShapeDtypeStruct((2, ROWS), F32),
            jax.ShapeDtypeStruct((2, COLS), F32),
        ],
        in_specs=[vmem, vmem, vmem],
        out_specs=[hbm, hbm, hbm],
        scratch_shapes=[dma((PAIRS + 2,))],
        compiler_params=pltpu.CompilerParams(vmem_limit_bytes=2**20),
        name="write",
    )(*results)


def solution(mesh):
    torus = Mesh(mesh.devices.reshape(2, 4, 2, 2, 4), AXES)
    in_specs = (P(ROW, COL), P(None, ROW, COL), P(None, ROW, COL), P(None, ROW), P(None, COL))
    out_specs = (P(COL, ROW), P(None, ROW), P(None, COL))
    return jax.shard_map(local, mesh=torus, in_specs=in_specs, out_specs=out_specs, check_vma=False)
```

```python
import jax
import jax.numpy as jnp
from jax import lax
from jax.experimental import pallas as pl
from jax.experimental.pallas import tpu as pltpu
from jax.sharding import Mesh
from jax.sharding import PartitionSpec as P

D = 8192
FF = 14336
AXES = ("yl", "x", "c", "yh", "z")
ROW = ("yl", "x", "c")
COL = ("yh", "z")
F32 = jnp.float32
BF16 = jnp.bfloat16
BY_MESH = pl.DeviceIdType.MESH

decay_rate = 0.5
learn_rate = 0.01
clip_limit = 1.0
tiny_eps = 1e-30

ROWS = 896
COLS = 1024
UNIT = 128
PAIRS = ROWS // UNIT
CHUNKS = PAIRS
LOCAL = 4
RINGS = CHUNKS + LOCAL
VMEM_LIMIT = 67043328 - 464 * 1024
LAG = 2
WIDE = 2 * UNIT
VALUES = WIDE
MESSAGE = VALUES + 16
SPAN = 250.0
HALF_LOG = 125.0 * 0.6931471805599453
ORDER = [0, LOCAL, 1, LOCAL + 1] + list(range(2, LOCAL)) + list(range(LOCAL + 2, CHUNKS))
LANES = 128
TILES = COLS // LANES
HALF = 1024
BLOCK = 256

COL_SUMS, ROW_SUMS, SUM_XC, SUM_YZ = 0, 16, 24, 32
STAT_SEMS = 48


def spread(row):
    return jnp.transpose(jnp.broadcast_to(row, (LANES, LANES)))


def put_code(ref, v):
    v = v.reshape(-1, 8, LANES)
    top = jnp.maximum(jnp.max(jnp.abs(v), axis=0) * 1.004, 1e-30).astype(BF16)
    factor = SPAN / top.astype(F32)
    q = jnp.exp2(jnp.abs(v) * factor - SPAN / 2.0)
    ref[:VALUES] = jnp.where(v < 0.0, -q, q).reshape(VALUES, LANES).astype(BF16)
    ref[VALUES:] = jnp.concatenate([top, top], axis=0)


def get_code(ref):
    top = ref[VALUES:].astype(F32)[:8]
    q = ref[:VALUES].astype(F32).reshape(-1, 8, LANES)
    v = (jnp.log(jnp.abs(q)) + HALF_LOG) * (top * (1.0 / (2.0 * HALF_LOG)))
    return jnp.where(q < 0.0, -v, v).reshape(VALUES, LANES)


def kernel(
    tok, wgt, grd, row_old, col_old,
    hid, row_out, col_out,
    rowf, colf, g, w, wown, wpart, t, p, e, r, away, come, kept,
    colacc, colsrc, rowsrc, colin, rowin,
    rn, cn, a, b, sumsrc, sum_xc, sum_yz,
    g_sem, w_sem, in_sem, st_s, st_r, ty_s, ty_r, nx_s, nx_r, fx_s, fx_r, tc_s, tc_r,
    wy_s, wy_r, rs_s, rs_r, fy_s, fy_r,
):
    yl = lax.axis_index("yl")
    x = lax.axis_index("x")
    c = lax.axis_index("c")
    yh = lax.axis_index("yh")
    z = lax.axis_index("z")
    y = 2 * yh + yl

    def at_row(q):
        return {"yl": lax.div(q, 8), "x": lax.rem(lax.div(q, 2), 4), "c": lax.rem(q, 2)}

    def at_col(q):
        return {"yh": lax.div(q, 4), "z": lax.rem(q, 4)}

    def at_xc(q):
        return {"x": lax.div(q, 2), "c": lax.rem(q, 2)}

    def at_yz(q):
        return {"yh": lax.div(q, 8), "yl": lax.rem(lax.div(q, 4), 2), "z": lax.rem(q, 4)}

    in_row = yl * 8 + x * 2 + c
    in_col = yh * 4 + z
    in_xc = x * 2 + c
    in_yz = y * 4 + z
    x_next = lax.rem(x + 1, 4)
    x_prev = lax.rem(x + 3, 4)
    x_far = lax.rem(x + 2, 4)
    sibling = {"c": 1 - c}
    yh_peer = {"yh": 1 - yh}

    def remote(src, dst, s, q, device):
        return pltpu.make_async_remote_copy(
            src_ref=src, dst_ref=dst, send_sem=s, recv_sem=q,
            device_id=device, device_id_type=BY_MESH,
        )

    def g_copy(m, k):
        rows = pl.ds(k * UNIT, UNIT)
        return pltpu.make_async_copy(grd.at[m, rows], g.at[m, rows], g_sem.at[m, k])

    for m in range(2):
        for k in range(PAIRS):
            g_copy(m, k).start()
    w_copies = [pltpu.make_async_copy(wgt.at[m], w.at[m], w_sem.at[m]) for m in range(2)]

    def rows_of(q, core):
        return pl.ds(pl.multiple_of((q * 2 + core) * 128, 128), 128)

    mine = rows_of(x, c)
    same = yl == yh
    slots = [jnp.where(same, yh, 2), jnp.where(same, 2, yh), 1 - yh]
    tok_copy = pltpu.make_async_copy(tok, t.at[slots[0], mine], in_sem.at[0])
    tok_copy.start()
    factor_copies = [
        pltpu.make_async_copy(row_old, rowf, in_sem.at[1]),
        pltpu.make_async_copy(col_old, colf, in_sem.at[2]),
    ]
    for copy in factor_copies + w_copies:
        copy.start()

    barrier = pltpu.get_barrier_semaphore()
    peers = [at_row(lax.rem(in_row + d, 16)) for d in range(1, 16)]
    peers += [at_yz(lax.rem(in_yz + d, 16)) for d in range(1, 16)]
    for device in peers:
        pl.semaphore_signal(barrier, inc=1, device_id=device, device_id_type=BY_MESH)
    colacc[...] = jnp.zeros_like(colacc)
    rn[...] = jnp.ones_like(rn)
    rowsrc[...] = jnp.zeros_like(rowsrc)
    for m in range(2):
        def squares(k, carry):
            g_copy(m, k).wait()
            rows = pl.ds(pl.multiple_of(k * UNIT, UNIT), UNIT)
            total = jnp.zeros((UNIT, LANES), F32)
            for j in range(TILES):
                v = g[m, rows, j * LANES:(j + 1) * LANES].astype(F32)
                v = v * v
                total = total + v
                colacc[m * TILES + j] += jnp.sum(v.reshape(UNIT // 8, 8, LANES), axis=0)
            rowsrc[pl.ds(m * PAIRS + k, 1), :] = jnp.sum(
                jnp.transpose(total), axis=0, keepdims=True
            )
            return carry

        lax.fori_loop(0, PAIRS, squares, 0)
    colsrc[...] = jnp.sum(colacc[...], axis=1)
    pl.semaphore_wait(barrier, len(peers))

    sent = []

    def give(src, slots, place, n, me, device_of):
        for d in range(1, n):
            q = lax.rem(me + d, n)
            copy = remote(src, slots.at[me], st_s.at[place + q], st_r.at[place + me], device_of(q))
            copy.start()
            sent.append(copy)
        slots[me] = src[...]

    def arrive(src, slots, place, n, me, device_of):
        for d in range(1, n):
            q = lax.rem(me + d, n)
            remote(src, slots.at[q], st_s.at[place + q], st_r.at[place + q], device_of(q)).wait_recv()

    def take(src, slots, place, n, me, device_of):
        arrive(src, slots, place, n, me, device_of)
        total = slots[0]
        for q in range(1, n):
            total = total + slots[q]
        return total

    give(rowsrc, rowin, ROW_SUMS, 8, in_col, at_col)
    give(colsrc, colin, COL_SUMS, 16, in_row, at_row)

    def near(f, side):
        rows = mine
        return remote(
            t.at[slots[f], rows], t.at[slots[f], rows], nx_s.at[f, side], nx_r.at[f, side],
            {"x": x_next if side == 0 else x_prev},
        )

    def near_in(f, side):
        rows = rows_of(x_prev if side == 0 else x_next, c)
        return remote(
            t.at[slots[f], rows], t.at[slots[f], rows], nx_s.at[f, side], nx_r.at[f, side],
            {"x": x_next if side == 0 else x_prev},
        )

    def half_rows(q, side):
        return pl.ds(pl.multiple_of((q * 2 + c) * 128 + 64 * side, 64), 64)

    def onward(f, side):
        rows = half_rows(x_prev if side == 0 else x_next, side)
        return remote(
            t.at[slots[f], rows], t.at[slots[f], rows], fx_s.at[f, side], fx_r.at[f, side],
            {"x": x_next if side == 0 else x_prev},
        )

    def onward_in(f, side):
        rows = half_rows(x_far, side)
        return remote(
            t.at[slots[f], rows], t.at[slots[f], rows], fx_s.at[f, side], fx_r.at[f, side],
            {"x": x_next if side == 0 else x_prev},
        )

    def to_sibling(q, f):
        rows = rows_of(q, c)
        return remote(t.at[slots[f], rows], t.at[slots[f], rows], tc_s.at[q, f], tc_r.at[q, f], sibling)

    def from_sibling(q, f):
        rows = rows_of(q, 1 - c)
        return remote(t.at[slots[f], rows], t.at[slots[f], rows], tc_s.at[q, f], tc_r.at[q, f], sibling)

    pair_send = remote(t.at[slots[0], mine], t.at[slots[0], mine], ty_s.at[0], ty_r.at[0], {"yl": 1 - yl})
    pair_in = remote(t.at[slots[1], mine], t.at[slots[1], mine], ty_s.at[0], ty_r.at[0], {"yl": 1 - yl})
    across_send = remote(
        t.at[slots[0], mine], t.at[yh, mine], ty_s.at[1], ty_r.at[1], {"yl": 1 - yl, "yh": 1 - yh}
    )
    across_in = remote(
        t.at[slots[2], mine], t.at[slots[2], mine], ty_s.at[1], ty_r.at[1], {"yl": 1 - yl, "yh": 1 - yh}
    )
    far_send = remote(t.at[slots[0], mine], t.at[yh, mine], ty_s.at[2], ty_r.at[2], yh_peer)
    far_in = remote(t.at[slots[2], mine], t.at[slots[2], mine], ty_s.at[2], ty_r.at[2], yh_peer)

    def share(f):
        for side in range(2):
            near(f, side).start()
        to_sibling(x, f).start()

    def pass_on(f):
        for side in range(2):
            near_in(f, side).wait_recv()
            onward(f, side).start()
        to_sibling(x_prev, f).start()
        to_sibling(x_next, f).start()

    def complete(f):
        for side in range(2):
            onward_in(f, side).wait_recv()
        to_sibling(x_far, f).start()

    def complete_sibling(f):
        for q in (x, x_prev, x_next, x_far):
            from_sibling(q, f).wait_recv()

    tok_copy.wait()
    pair_send.start()

    @pl.when(jnp.logical_not(same))
    def _():
        across_send.start()
        far_send.start()

    share(0)
    for copy in factor_copies:
        copy.wait()

    for copy in w_copies:
        copy.wait()
    sumsrc[...] = jnp.zeros_like(sumsrc)

    row_total = take(rowsrc, rowin, ROW_SUMS, 8, in_col, at_col)
    for m in range(2):
        for k in range(PAIRS):
            i = m * PAIRS + k
            rn[i:i + 1] = decay_rate * rowf[m:m + 1, k * UNIT:(k + 1) * UNIT] + (1.0 - decay_rate) * (
                row_total[i:i + 1] / D + tiny_eps
            )
            row_out[m:m + 1, k * UNIT:(k + 1) * UNIT] = rn[i:i + 1]
    col_total = take(colsrc, colin, COL_SUMS, 16, in_row, at_row)
    for m in range(2):
        for j in range(TILES):
            i = m * TILES + j
            cn[i:i + 1] = decay_rate * colf[m:m + 1, j * LANES:(j + 1) * LANES] + (1.0 - decay_rate) * (
                col_total[i:i + 1] / FF + tiny_eps
            )
            col_out[m:m + 1, j * LANES:(j + 1) * LANES] = cn[i:i + 1]

    a[...] = 1.0 / rn[...]
    b[...] = 1.0 / cn[...]
    for m in range(2):
        def norms(k, carry):
            rows = pl.ds(pl.multiple_of(k * UNIT, UNIT), UNIT)
            total = jnp.zeros((UNIT, LANES), F32)
            for j in range(TILES):
                v = g[m, rows, j * LANES:(j + 1) * LANES].astype(F32)
                total = total + v * v * b[m * TILES + j:m * TILES + j + 1]
            total = total * spread(a[pl.ds(m * PAIRS + k, 1), :])
            return carry + jnp.sum(total.reshape(UNIT // 8, 8, LANES), axis=0)

        parts = lax.fori_loop(0, PAIRS, norms, jnp.zeros((8, LANES), F32))
        sumsrc[0, m:m + 1] = jnp.sum(parts, axis=0, keepdims=True)
        sumsrc[0, 2 + m:3 + m] = jnp.sum(rn[m * PAIRS:(m + 1) * PAIRS], axis=0, keepdims=True)

    give(sumsrc.at[0], sum_xc, SUM_XC, 8, in_xc, at_xc)
    pass_on(0)
    pair_in.wait_recv()
    share(1)
    sumsrc[1] = take(sumsrc.at[0], sum_xc, SUM_XC, 8, in_xc, at_xc)
    give(sumsrc.at[1], sum_yz, SUM_YZ, 16, in_yz, at_yz)
    complete(0)
    total = take(sumsrc.at[1], sum_yz, SUM_YZ, 16, in_yz, at_yz)

    for m in range(2):
        row_mean = jnp.sum(total[2 + m:3 + m], axis=1, keepdims=True) / (8.0 * FF)
        norm_total = jnp.sum(total[m:m + 1], axis=1, keepdims=True) * row_mean
        clip_scale = jnp.maximum(1.0, jnp.sqrt(norm_total / (FF * D)) / clip_limit)
        scale = learn_rate * jnp.sqrt(row_mean) / clip_scale
        a[m * PAIRS:(m + 1) * PAIRS] = scale / jnp.sqrt(rn[m * PAIRS:(m + 1) * PAIRS])
    b[...] = 1.0 / jnp.sqrt(cn[...])

    def weight_send(k):
        return remote(wown.at[k], wpart.at[k - LOCAL], wy_s.at[k], wy_r.at[k], yh_peer)

    def update(i, carry):
        k = ORDER[-1]
        for q in range(CHUNKS - 1):
            k = jnp.where(i == q, ORDER[q], k)
        rows = pl.ds(pl.multiple_of(k * UNIT, UNIT), UNIT)
        for m in range(2):
            factor = spread(a[pl.ds(m * PAIRS + k, 1), :])
            for j in range(TILES):
                cols = slice(j * LANES, (j + 1) * LANES)
                step = g[m, rows, cols].astype(F32) * factor * b[m * TILES + j:m * TILES + j + 1]
                wown[k, m * UNIT:(m + 1) * UNIT, cols] = (w[m, rows, cols].astype(F32) - step).astype(BF16)

        @pl.when(k >= LOCAL)
        def _():
            weight_send(k).start()

        return carry

    lax.fori_loop(0, 2, update, 0)
    complete_sibling(0)

    right = lax.rem(z + 1, 4)
    left = lax.rem(z + 3, 4)

    def block_of(side, s):
        return lax.rem(z + 3 - s, 4) if side == 0 else lax.rem(z + 1 + s, 4)

    def ring_copy(n, s, side):
        target = right if side == 0 else left
        return remote(
            e.at[n, s, side], r.at[n, s, side],
            rs_s.at[n, s, side], rs_r.at[n, s, side], {"z": target},
        )

    def times(block, slot, weights):
        tokens = t[slot, pl.ds(pl.multiple_of(block * BLOCK, BLOCK), BLOCK), :]
        return lax.dot_general(
            tokens, weights[...], (((1,), (1,)), ((), ())), preferred_element_type=F32
        )

    def arrange(v):
        parts = []
        for side in range(2):
            rows = slice(side * (BLOCK // 2), (side + 1) * (BLOCK // 2))
            parts.append(jnp.concatenate([v[rows, :UNIT], v[rows, UNIT:]], axis=0))
        return parts

    def begin(n, d, parts):
        if d in (3, 1):
            side = 0 if d == 3 else 1
            put_code(e.at[n, 0, side], parts[side])
            ring_copy(n, 0, side).start()

    def local_products(n):
        k = jnp.where(n < LOCAL, n, n - LOCAL)
        slot = jnp.where(n < LOCAL, slots[0], slots[1])
        for d in (3, 1, 2, 0):
            block = lax.rem(z + d, 4)
            parts = arrange(times(block, slot, wown.at[k]))
            for side in range(2):
                p[n, block, side] = parts[side]
            begin(n, d, parts)

    def own_products(n):
        for d in (3, 1, 2, 0):
            block = lax.rem(z + d, 4)
            parts = arrange(times(block, yh, wown.at[n - LOCAL]))
            for side in range(2):
                p[n, block, side] = parts[side]

    def other_products(n):
        for d in (3, 1, 2, 0):
            block = lax.rem(z + d, 4)
            parts = arrange(times(block, 1 - yh, wpart.at[n - 2 * LOCAL]))
            for side in range(2):
                parts[side] = parts[side] + p[n, block, side]
                p[n, block, side] = parts[side]
            begin(n, d, parts)

    def ring_step(n, s):
        for side in range(2):
            ring_copy(n, s - 1, side).wait_recv()
            put_code(e.at[n, s, side], p[n, block_of(side, s), side] + get_code(r.at[n, s - 1, side]))
            ring_copy(n, s, side).start()

    def hidden(k, side, v):
        gate = v[:UNIT]
        up = v[UNIT:]
        rows = slice(side * (BLOCK // 2), (side + 1) * (BLOCK // 2))
        hid[k, rows] = (gate / (1.0 + jnp.exp(-gate)) * up).astype(BF16)

    def final_send(n):
        return remote(away.at[n], come.at[n], fy_s.at[n], fy_r.at[n], yh_peer)

    def leaves(n):
        return (jnp.logical_not(same) & (n < LOCAL)) | (same & (n >= LOCAL) & (n < 2 * LOCAL))

    def finish(n):
        for side in range(2):
            ring_copy(n, 2, side).wait_recv()
            v = p[n, z, side] + get_code(r.at[n, 2, side])

            @pl.when(leaves(n))
            def _():
                put_code(away.at[lax.rem(n, LOCAL), side], v)

            @pl.when(jnp.logical_not(leaves(n)) & (n < 2 * LOCAL))
            def _():
                kept[lax.rem(n, LOCAL), side] = v

            @pl.when(n >= 2 * LOCAL)
            def _():
                hidden(n - LOCAL, side, v)

        @pl.when(leaves(n))
        def _():
            final_send(lax.rem(n, LOCAL)).start()

    def work(n, carry):
        @pl.when(n < 2 * LOCAL)
        def _():
            local_products(n)

        @pl.when((n >= 2 * LOCAL) & (n < RINGS))
        def _():
            own_products(n)

        @pl.when(n < PAIRS - 3)
        def _():
            lax.fori_loop(jnp.where(n == 0, 2, n + 3), n + 4, update, 0)

        for s in (1, 2):
            @pl.when((n >= s * LAG) & (n < RINGS + s * LAG))
            def _():
                ring_step(n - s * LAG, s)

        @pl.when(n >= 3 * LAG)
        def _():
            finish(n - 3 * LAG)

        @pl.when(n == 1)
        def _():
            pass_on(1)

        @pl.when(n == 2)
        def _():
            @pl.when(same)
            def _():
                far_in.wait_recv()

            @pl.when(jnp.logical_not(same))
            def _():
                across_in.wait_recv()

            share(2)

        @pl.when(n == LOCAL + 1)
        def _():
            pass_on(2)

        @pl.when(n == LOCAL - 1)
        def _():
            complete(1)
            complete_sibling(1)

        @pl.when(n == 2 * LOCAL)
        def _():
            complete(2)
            complete_sibling(2)

        @pl.when((n >= 2 * LOCAL) & (n < RINGS))
        def _():
            weight_send(n - LOCAL).wait_recv()
            other_products(n)

        return carry

    lax.fori_loop(0, RINGS + 3 * LAG, work, 0)

    def last(n, carry):
        final_send(n).wait_recv()
        for side in range(2):
            hidden(n, side, kept[n, side] + get_code(come.at[n, side]))
        return carry

    lax.fori_loop(0, LOCAL, last, 0)

    for copy in sent:
        copy.wait_send()
    pair_send.wait_send()

    @pl.when(jnp.logical_not(same))
    def _():
        across_send.wait_send()
        far_send.wait_send()

    for f in range(3):
        for side in range(2):
            near(f, side).wait_send()
            onward(f, side).wait_send()
        for q in range(4):
            to_sibling(q, f).wait_send()

    def drain(n, carry):
        @pl.when(n >= 2 * LOCAL)
        def _():
            weight_send(n - LOCAL).wait_send()

        @pl.when(n < LOCAL)
        def _():
            final_send(n).wait_send()

        for s in range(3):
            for side in range(2):
                ring_copy(n, s, side).wait_send()
        return carry

    lax.fori_loop(0, RINGS, drain, 0)


def writer(hid, row_new, col_new, hid_out, row_out, col_out, sem):
    copies = [
        pltpu.make_async_copy(hid.at[k], hid_out.at[:, k * UNIT:(k + 1) * UNIT], sem.at[k])
        for k in range(PAIRS)
    ]
    copies += [
        pltpu.make_async_copy(row_new, row_out, sem.at[PAIRS]),
        pltpu.make_async_copy(col_new, col_out, sem.at[PAIRS + 1]),
    ]
    for copy in copies:
        copy.start()
    for copy in copies:
        copy.wait()


def local(tokens, weights, gradients, row_factors, col_factors):
    vmem = pl.BlockSpec(memory_space=pltpu.VMEM)
    hbm = pl.BlockSpec(memory_space=pl.ANY)
    dma = pltpu.SemaphoreType.DMA
    scratch = [
        pltpu.VMEM((2, ROWS), F32),
        pltpu.VMEM((2, COLS), F32),
        pltpu.VMEM((2, ROWS, COLS), BF16),
        pltpu.VMEM((2, ROWS, COLS), BF16),
        pltpu.VMEM((CHUNKS, WIDE, COLS), BF16),
        pltpu.VMEM((CHUNKS - LOCAL, WIDE, COLS), BF16),
        pltpu.VMEM((3, HALF, COLS), BF16),
        pltpu.VMEM((RINGS, 4, 2, VALUES, LANES), F32),
        pltpu.VMEM((RINGS, 3, 2, MESSAGE, LANES), BF16),
        pltpu.VMEM((RINGS, 3, 2, MESSAGE, LANES), BF16),
        pltpu.VMEM((LOCAL, 2, MESSAGE, LANES), BF16),
        pltpu.VMEM((LOCAL, 2, MESSAGE, LANES), BF16),
        pltpu.VMEM((LOCAL, 2, VALUES, LANES), F32),
        pltpu.VMEM((16, 8, LANES), F32),
        pltpu.VMEM((16, LANES), F32),
        pltpu.VMEM((16, LANES), F32),
        pltpu.VMEM((16, 16, LANES), F32),
        pltpu.VMEM((8, 16, LANES), F32),
        pltpu.VMEM((16, LANES), F32),
        pltpu.VMEM((16, LANES), F32),
        pltpu.VMEM((16, LANES), F32),
        pltpu.VMEM((16, LANES), F32),
        pltpu.VMEM((2, 8, LANES), F32),
        pltpu.VMEM((8, 8, LANES), F32),
        pltpu.VMEM((16, 8, LANES), F32),
        dma((2, PAIRS)), dma((2,)), dma((3,)), dma((STAT_SEMS,)), dma((STAT_SEMS,)),
        dma((3,)), dma((3,)), dma((3, 2)), dma((3, 2)), dma((3, 2)), dma((3, 2)), dma((4, 3)), dma((4, 3)),
        dma((CHUNKS,)), dma((CHUNKS,)), dma((RINGS, 3, 2)), dma((RINGS, 3, 2)),
        dma((LOCAL,)), dma((LOCAL,)),
    ]
    results = pl.pallas_call(
        kernel,
        out_shape=[
            pltpu.VMEM((PAIRS, BLOCK, UNIT), BF16),
            pltpu.VMEM((2, ROWS), F32),
            pltpu.VMEM((2, COLS), F32),
        ],
        in_specs=[hbm] * 5,
        out_specs=[vmem, vmem, vmem],
        scratch_shapes=scratch,
        compiler_params=pltpu.CompilerParams(
            collective_id=0, has_side_effects=True, vmem_limit_bytes=VMEM_LIMIT
        ),
        name="step",
    )(tokens, weights, gradients, row_factors, col_factors)
    return pl.pallas_call(
        writer,
        out_shape=[
            jax.ShapeDtypeStruct((BLOCK, ROWS), BF16),
            jax.ShapeDtypeStruct((2, ROWS), F32),
            jax.ShapeDtypeStruct((2, COLS), F32),
        ],
        in_specs=[vmem, vmem, vmem],
        out_specs=[hbm, hbm, hbm],
        scratch_shapes=[dma((PAIRS + 2,))],
        compiler_params=pltpu.CompilerParams(vmem_limit_bytes=2**20),
        name="write",
    )(*results)


def solution(mesh):
    torus = Mesh(mesh.devices.reshape(2, 4, 2, 2, 4), AXES)
    in_specs = (P(ROW, COL), P(None, ROW, COL), P(None, ROW, COL), P(None, ROW), P(None, COL))
    out_specs = (P(COL, ROW), P(None, ROW), P(None, COL))
    return jax.shard_map(local, mesh=torus, in_specs=in_specs, out_specs=out_specs, check_vma=False)
```

```python
import jax
import jax.numpy as jnp
from jax import lax
from jax.experimental import pallas as pl
from jax.experimental.pallas import tpu as pltpu
from jax.sharding import Mesh
from jax.sharding import PartitionSpec as P

D = 8192
FF = 14336
AXES = ("yl", "x", "c", "yh", "z")
ROW = ("yl", "x", "c")
COL = ("yh", "z")
F32 = jnp.float32
BF16 = jnp.bfloat16
BY_MESH = pl.DeviceIdType.MESH

decay_rate = 0.5
learn_rate = 0.01
clip_limit = 1.0
tiny_eps = 1e-30

ROWS = 896
COLS = 1024
UNIT = 128
PAIRS = ROWS // UNIT
CHUNKS = PAIRS
LOCAL = 4
RINGS = CHUNKS + LOCAL
VMEM_LIMIT = 67043328 - 464 * 1024
LAG = 2
WIDE = 2 * UNIT
VALUES = WIDE
MESSAGE = VALUES + 16
SPAN = 250.0
HALF_LOG = 125.0 * 0.6931471805599453
ORDER = [0, LOCAL, 1, LOCAL + 1] + list(range(2, LOCAL)) + list(range(LOCAL + 2, CHUNKS))
LANES = 128
TILES = COLS // LANES
HALF = 1024
BLOCK = 256

COL_SUMS, ROW_SUMS, SUM_XC, SUM_YZ = 0, 16, 24, 32
STAT_SEMS = 48


def spread(row):
    return jnp.transpose(jnp.broadcast_to(row, (LANES, LANES)))


def put_code(ref, v):
    v = v.reshape(-1, 8, LANES)
    top = jnp.maximum(jnp.max(jnp.abs(v), axis=0) * 1.004, 1e-30).astype(BF16)
    factor = SPAN / top.astype(F32)
    q = jnp.exp2(jnp.abs(v) * factor - SPAN / 2.0)
    ref[:VALUES] = jnp.where(v < 0.0, -q, q).reshape(VALUES, LANES).astype(BF16)
    ref[VALUES:] = jnp.concatenate([top, top], axis=0)


def get_code(ref):
    top = ref[VALUES:].astype(F32)[:8]
    q = ref[:VALUES].astype(F32).reshape(-1, 8, LANES)
    v = (jnp.log(jnp.abs(q)) + HALF_LOG) * (top * (1.0 / (2.0 * HALF_LOG)))
    return jnp.where(q < 0.0, -v, v).reshape(VALUES, LANES)


def kernel(
    tok, wgt, grd, row_old, col_old,
    hid, row_out, col_out,
    rowf, colf, g, w, wown, wpart, t, p, e, r, away, come, kept,
    colacc, colsrc, rowsrc, colin, rowin,
    rn, cn, a, b, sumsrc, sum_xc, sum_yz,
    g_sem, w_sem, in_sem, st_s, st_r, ty_s, ty_r, nx_s, nx_r, fx_s, fx_r, tc_s, tc_r,
    wy_s, wy_r, rs_s, rs_r, fy_s, fy_r,
):
    yl = lax.axis_index("yl")
    x = lax.axis_index("x")
    c = lax.axis_index("c")
    yh = lax.axis_index("yh")
    z = lax.axis_index("z")
    y = 2 * yh + yl

    def at_row(q):
        return {"yl": lax.div(q, 8), "x": lax.rem(lax.div(q, 2), 4), "c": lax.rem(q, 2)}

    def at_col(q):
        return {"yh": lax.div(q, 4), "z": lax.rem(q, 4)}

    def at_xc(q):
        return {"x": lax.div(q, 2), "c": lax.rem(q, 2)}

    def at_yz(q):
        return {"yh": lax.div(q, 8), "yl": lax.rem(lax.div(q, 4), 2), "z": lax.rem(q, 4)}

    in_row = yl * 8 + x * 2 + c
    in_col = yh * 4 + z
    in_xc = x * 2 + c
    in_yz = y * 4 + z
    x_next = lax.rem(x + 1, 4)
    x_prev = lax.rem(x + 3, 4)
    x_far = lax.rem(x + 2, 4)
    sibling = {"c": 1 - c}
    yh_peer = {"yh": 1 - yh}

    def remote(src, dst, s, q, device):
        return pltpu.make_async_remote_copy(
            src_ref=src, dst_ref=dst, send_sem=s, recv_sem=q,
            device_id=device, device_id_type=BY_MESH,
        )

    def g_copy(m, k):
        rows = pl.ds(k * UNIT, UNIT)
        return pltpu.make_async_copy(grd.at[m, rows], g.at[m, rows], g_sem.at[m, k])

    for m in range(2):
        for k in range(PAIRS):
            g_copy(m, k).start()
    w_copies = [pltpu.make_async_copy(wgt.at[m], w.at[m], w_sem.at[m]) for m in range(2)]

    def rows_of(q, core):
        return pl.ds(pl.multiple_of((q * 2 + core) * 128, 128), 128)

    mine = rows_of(x, c)
    same = yl == yh
    slots = [jnp.where(same, yh, 2), jnp.where(same, 2, yh), 1 - yh]
    tok_copy = pltpu.make_async_copy(tok, t.at[slots[0], mine], in_sem.at[0])
    tok_copy.start()
    factor_copies = [
        pltpu.make_async_copy(row_old, rowf, in_sem.at[1]),
        pltpu.make_async_copy(col_old, colf, in_sem.at[2]),
    ]
    for copy in factor_copies + w_copies:
        copy.start()

    barrier = pltpu.get_barrier_semaphore()
    peers = [at_row(lax.rem(in_row + d, 16)) for d in range(1, 16)]
    peers += [at_yz(lax.rem(in_yz + d, 16)) for d in range(1, 16)]
    for device in peers:
        pl.semaphore_signal(barrier, inc=1, device_id=device, device_id_type=BY_MESH)
    colacc[...] = jnp.zeros_like(colacc)
    rn[...] = jnp.ones_like(rn)
    rowsrc[...] = jnp.zeros_like(rowsrc)
    for m in range(2):
        def squares(k, carry):
            g_copy(m, k).wait()
            rows = pl.ds(pl.multiple_of(k * UNIT, UNIT), UNIT)
            total = jnp.zeros((UNIT, LANES), F32)
            for j in range(TILES):
                v = g[m, rows, j * LANES:(j + 1) * LANES].astype(F32)
                v = v * v
                total = total + v
                colacc[m * TILES + j] += jnp.sum(v.reshape(UNIT // 8, 8, LANES), axis=0)
            rowsrc[pl.ds(m * PAIRS + k, 1), :] = jnp.sum(
                jnp.transpose(total), axis=0, keepdims=True
            )
            return carry

        lax.fori_loop(0, PAIRS, squares, 0)
    colsrc[...] = jnp.sum(colacc[...], axis=1)
    pl.semaphore_wait(barrier, len(peers))

    sent = []

    def give(src, slots, place, n, me, device_of):
        for d in range(1, n):
            q = lax.rem(me + d, n)
            copy = remote(src, slots.at[me], st_s.at[place + q], st_r.at[place + me], device_of(q))
            copy.start()
            sent.append(copy)
        slots[me] = src[...]

    def arrive(src, slots, place, n, me, device_of):
        for d in range(1, n):
            q = lax.rem(me + d, n)
            remote(src, slots.at[q], st_s.at[place + q], st_r.at[place + q], device_of(q)).wait_recv()

    def take(src, slots, place, n, me, device_of):
        arrive(src, slots, place, n, me, device_of)
        total = slots[0]
        for q in range(1, n):
            total = total + slots[q]
        return total

    give(rowsrc, rowin, ROW_SUMS, 8, in_col, at_col)
    give(colsrc, colin, COL_SUMS, 16, in_row, at_row)

    def near(f, side):
        rows = mine
        return remote(
            t.at[slots[f], rows], t.at[slots[f], rows], nx_s.at[f, side], nx_r.at[f, side],
            {"x": x_next if side == 0 else x_prev},
        )

    def near_in(f, side):
        rows = rows_of(x_prev if side == 0 else x_next, c)
        return remote(
            t.at[slots[f], rows], t.at[slots[f], rows], nx_s.at[f, side], nx_r.at[f, side],
            {"x": x_next if side == 0 else x_prev},
        )

    def half_rows(q, side):
        return pl.ds(pl.multiple_of((q * 2 + c) * 128 + 64 * side, 64), 64)

    def onward(f, side):
        rows = half_rows(x_prev if side == 0 else x_next, side)
        return remote(
            t.at[slots[f], rows], t.at[slots[f], rows], fx_s.at[f, side], fx_r.at[f, side],
            {"x": x_next if side == 0 else x_prev},
        )

    def onward_in(f, side):
        rows = half_rows(x_far, side)
        return remote(
            t.at[slots[f], rows], t.at[slots[f], rows], fx_s.at[f, side], fx_r.at[f, side],
            {"x": x_next if side == 0 else x_prev},
        )

    def to_sibling(q, f):
        rows = rows_of(q, c)
        return remote(t.at[slots[f], rows], t.at[slots[f], rows], tc_s.at[q, f], tc_r.at[q, f], sibling)

    def from_sibling(q, f):
        rows = rows_of(q, 1 - c)
        return remote(t.at[slots[f], rows], t.at[slots[f], rows], tc_s.at[q, f], tc_r.at[q, f], sibling)

    pair_send = remote(t.at[slots[0], mine], t.at[slots[0], mine], ty_s.at[0], ty_r.at[0], {"yl": 1 - yl})
    pair_in = remote(t.at[slots[1], mine], t.at[slots[1], mine], ty_s.at[0], ty_r.at[0], {"yl": 1 - yl})
    across_send = remote(
        t.at[slots[0], mine], t.at[yh, mine], ty_s.at[1], ty_r.at[1], {"yl": 1 - yl, "yh": 1 - yh}
    )
    across_in = remote(
        t.at[slots[2], mine], t.at[slots[2], mine], ty_s.at[1], ty_r.at[1], {"yl": 1 - yl, "yh": 1 - yh}
    )
    far_send = remote(t.at[slots[0], mine], t.at[yh, mine], ty_s.at[2], ty_r.at[2], yh_peer)
    far_in = remote(t.at[slots[2], mine], t.at[slots[2], mine], ty_s.at[2], ty_r.at[2], yh_peer)

    def share(f):
        for side in range(2):
            near(f, side).start()
        to_sibling(x, f).start()

    def pass_on(f):
        for side in range(2):
            near_in(f, side).wait_recv()
            onward(f, side).start()
        to_sibling(x_prev, f).start()
        to_sibling(x_next, f).start()

    def complete(f):
        for side in range(2):
            onward_in(f, side).wait_recv()
        to_sibling(x_far, f).start()

    def complete_sibling(f):
        for q in (x, x_prev, x_next, x_far):
            from_sibling(q, f).wait_recv()

    tok_copy.wait()
    pair_send.start()

    @pl.when(jnp.logical_not(same))
    def _():
        across_send.start()
        far_send.start()

    share(0)
    for copy in factor_copies:
        copy.wait()

    for copy in w_copies:
        copy.wait()
    sumsrc[...] = jnp.zeros_like(sumsrc)

    row_total = take(rowsrc, rowin, ROW_SUMS, 8, in_col, at_col)
    for m in range(2):
        for k in range(PAIRS):
            i = m * PAIRS + k
            rn[i:i + 1] = decay_rate * rowf[m:m + 1, k * UNIT:(k + 1) * UNIT] + (1.0 - decay_rate) * (
                row_total[i:i + 1] / D + tiny_eps
            )
            row_out[m:m + 1, k * UNIT:(k + 1) * UNIT] = rn[i:i + 1]
    col_total = take(colsrc, colin, COL_SUMS, 16, in_row, at_row)
    for m in range(2):
        for j in range(TILES):
            i = m * TILES + j
            cn[i:i + 1] = decay_rate * colf[m:m + 1, j * LANES:(j + 1) * LANES] + (1.0 - decay_rate) * (
                col_total[i:i + 1] / FF + tiny_eps
            )
            col_out[m:m + 1, j * LANES:(j + 1) * LANES] = cn[i:i + 1]

    a[...] = 1.0 / rn[...]
    b[...] = 1.0 / cn[...]
    for m in range(2):
        def norms(k, carry):
            rows = pl.ds(pl.multiple_of(k * UNIT, UNIT), UNIT)
            total = jnp.zeros((UNIT, LANES), F32)
            for j in range(TILES):
                v = g[m, rows, j * LANES:(j + 1) * LANES].astype(F32)
                total = total + v * v * b[m * TILES + j:m * TILES + j + 1]
            total = total * spread(a[pl.ds(m * PAIRS + k, 1), :])
            return carry + jnp.sum(total.reshape(UNIT // 8, 8, LANES), axis=0)

        parts = lax.fori_loop(0, PAIRS, norms, jnp.zeros((8, LANES), F32))
        sumsrc[0, m:m + 1] = jnp.sum(parts, axis=0, keepdims=True)
        sumsrc[0, 2 + m:3 + m] = jnp.sum(rn[m * PAIRS:(m + 1) * PAIRS], axis=0, keepdims=True)

    give(sumsrc.at[0], sum_xc, SUM_XC, 8, in_xc, at_xc)
    pass_on(0)
    pair_in.wait_recv()
    share(1)
    sumsrc[1] = take(sumsrc.at[0], sum_xc, SUM_XC, 8, in_xc, at_xc)
    give(sumsrc.at[1], sum_yz, SUM_YZ, 16, in_yz, at_yz)
    complete(0)
    total = take(sumsrc.at[1], sum_yz, SUM_YZ, 16, in_yz, at_yz)

    for m in range(2):
        row_mean = jnp.sum(total[2 + m:3 + m], axis=1, keepdims=True) / (8.0 * FF)
        norm_total = jnp.sum(total[m:m + 1], axis=1, keepdims=True) * row_mean
        clip_scale = jnp.maximum(1.0, jnp.sqrt(norm_total / (FF * D)) / clip_limit)
        scale = learn_rate * jnp.sqrt(row_mean) / clip_scale
        a[m * PAIRS:(m + 1) * PAIRS] = scale / jnp.sqrt(rn[m * PAIRS:(m + 1) * PAIRS])
    b[...] = 1.0 / jnp.sqrt(cn[...])

    def weight_send(k):
        return remote(wown.at[k], wpart.at[k - LOCAL], wy_s.at[k], wy_r.at[k], yh_peer)

    def update(i, carry):
        k = ORDER[-1]
        for q in range(CHUNKS - 1):
            k = jnp.where(i == q, ORDER[q], k)
        rows = pl.ds(pl.multiple_of(k * UNIT, UNIT), UNIT)
        for m in range(2):
            factor = spread(a[pl.ds(m * PAIRS + k, 1), :])
            for j in range(TILES):
                cols = slice(j * LANES, (j + 1) * LANES)
                step = g[m, rows, cols].astype(F32) * factor * b[m * TILES + j:m * TILES + j + 1]
                wown[k, m * UNIT:(m + 1) * UNIT, cols] = (w[m, rows, cols].astype(F32) - step).astype(BF16)

        @pl.when(k >= LOCAL)
        def _():
            weight_send(k).start()

        return carry

    lax.fori_loop(0, 2, update, 0)
    complete_sibling(0)

    right = lax.rem(z + 1, 4)
    left = lax.rem(z + 3, 4)

    def block_of(side, s):
        return lax.rem(z + 3 - s, 4) if side == 0 else lax.rem(z + 1 + s, 4)

    def ring_copy(n, s, side):
        target = right if side == 0 else left
        return remote(
            e.at[n, s, side], r.at[n, s, side],
            rs_s.at[n, s, side], rs_r.at[n, s, side], {"z": target},
        )

    def times(block, slot, weights):
        tokens = t[slot, pl.ds(pl.multiple_of(block * BLOCK, BLOCK), BLOCK), :]
        return lax.dot_general(
            tokens, weights[...], (((1,), (1,)), ((), ())), preferred_element_type=F32
        )

    def arrange(v):
        parts = []
        for side in range(2):
            rows = slice(side * (BLOCK // 2), (side + 1) * (BLOCK // 2))
            parts.append(jnp.concatenate([v[rows, :UNIT], v[rows, UNIT:]], axis=0))
        return parts

    def begin(n, d, parts):
        if d in (3, 1):
            side = 0 if d == 3 else 1
            put_code(e.at[n, 0, side], parts[side])
            ring_copy(n, 0, side).start()

    def local_products(n):
        k = jnp.where(n < LOCAL, n, n - LOCAL)
        slot = jnp.where(n < LOCAL, slots[0], slots[1])
        for d in (3, 1, 2, 0):
            block = lax.rem(z + d, 4)
            parts = arrange(times(block, slot, wown.at[k]))
            for side in range(2):
                p[n, block, side] = parts[side]
            begin(n, d, parts)

    def own_products(n):
        for d in (3, 1, 2, 0):
            block = lax.rem(z + d, 4)
            parts = arrange(times(block, yh, wown.at[n - LOCAL]))
            for side in range(2):
                p[n, block, side] = parts[side]

    def other_products(n):
        for d in (3, 1, 2, 0):
            block = lax.rem(z + d, 4)
            parts = arrange(times(block, 1 - yh, wpart.at[n - 2 * LOCAL]))
            for side in range(2):
                parts[side] = parts[side] + p[n, block, side]
                p[n, block, side] = parts[side]
            begin(n, d, parts)

    def ring_step(n, s):
        for side in range(2):
            ring_copy(n, s - 1, side).wait_recv()
            put_code(e.at[n, s, side], p[n, block_of(side, s), side] + get_code(r.at[n, s - 1, side]))
            ring_copy(n, s, side).start()

    def hidden(k, side, v):
        gate = v[:UNIT]
        up = v[UNIT:]
        rows = slice(side * (BLOCK // 2), (side + 1) * (BLOCK // 2))
        hid[k, rows] = (gate / (1.0 + jnp.exp(-gate)) * up).astype(BF16)

    def final_send(n):
        return remote(away.at[n], come.at[n], fy_s.at[n], fy_r.at[n], yh_peer)

    def leaves(n):
        return (jnp.logical_not(same) & (n < LOCAL)) | (same & (n >= LOCAL) & (n < 2 * LOCAL))

    def finish(n):
        for side in range(2):
            ring_copy(n, 2, side).wait_recv()
            v = p[n, z, side] + get_code(r.at[n, 2, side])

            @pl.when(leaves(n))
            def _():
                put_code(away.at[lax.rem(n, LOCAL), side], v)

            @pl.when(jnp.logical_not(leaves(n)) & (n < 2 * LOCAL))
            def _():
                kept[lax.rem(n, LOCAL), side] = v

            @pl.when(n >= 2 * LOCAL)
            def _():
                hidden(n - LOCAL, side, v)

        @pl.when(leaves(n))
        def _():
            final_send(lax.rem(n, LOCAL)).start()

    def work(n, carry):
        @pl.when(n < 2 * LOCAL)
        def _():
            local_products(n)

        @pl.when((n >= 2 * LOCAL) & (n < RINGS))
        def _():
            own_products(n)

        @pl.when(n < PAIRS - 3)
        def _():
            lax.fori_loop(jnp.where(n == 0, 2, n + 3), n + 4, update, 0)

        for s in (1, 2):
            @pl.when((n >= s * LAG) & (n < RINGS + s * LAG))
            def _():
                ring_step(n - s * LAG, s)

        @pl.when(n >= 3 * LAG)
        def _():
            finish(n - 3 * LAG)

        @pl.when(n == 0)
        def _():
            pass_on(1)

        @pl.when(n == 4)
        def _():
            @pl.when(same)
            def _():
                far_in.wait_recv()

            @pl.when(jnp.logical_not(same))
            def _():
                across_in.wait_recv()

            share(2)

        @pl.when(n == LOCAL + 2)
        def _():
            pass_on(2)

        @pl.when(n == LOCAL - 1)
        def _():
            complete(1)
            complete_sibling(1)

        @pl.when(n == 2 * LOCAL)
        def _():
            complete(2)
            complete_sibling(2)

        @pl.when((n >= 2 * LOCAL) & (n < RINGS))
        def _():
            weight_send(n - LOCAL).wait_recv()
            other_products(n)

        return carry

    lax.fori_loop(0, RINGS + 3 * LAG, work, 0)

    def last(n, carry):
        final_send(n).wait_recv()
        for side in range(2):
            hidden(n, side, kept[n, side] + get_code(come.at[n, side]))
        return carry

    lax.fori_loop(0, LOCAL, last, 0)

    for copy in sent:
        copy.wait_send()
    pair_send.wait_send()

    @pl.when(jnp.logical_not(same))
    def _():
        across_send.wait_send()
        far_send.wait_send()

    for f in range(3):
        for side in range(2):
            near(f, side).wait_send()
            onward(f, side).wait_send()
        for q in range(4):
            to_sibling(q, f).wait_send()

    def drain(n, carry):
        @pl.when(n >= 2 * LOCAL)
        def _():
            weight_send(n - LOCAL).wait_send()

        @pl.when(n < LOCAL)
        def _():
            final_send(n).wait_send()

        for s in range(3):
            for side in range(2):
                ring_copy(n, s, side).wait_send()
        return carry

    lax.fori_loop(0, RINGS, drain, 0)


def writer(hid, row_new, col_new, hid_out, row_out, col_out, sem):
    copies = [
        pltpu.make_async_copy(hid.at[k], hid_out.at[:, k * UNIT:(k + 1) * UNIT], sem.at[k])
        for k in range(PAIRS)
    ]
    copies += [
        pltpu.make_async_copy(row_new, row_out, sem.at[PAIRS]),
        pltpu.make_async_copy(col_new, col_out, sem.at[PAIRS + 1]),
    ]
    for copy in copies:
        copy.start()
    for copy in copies:
        copy.wait()


def local(tokens, weights, gradients, row_factors, col_factors):
    vmem = pl.BlockSpec(memory_space=pltpu.VMEM)
    hbm = pl.BlockSpec(memory_space=pl.ANY)
    dma = pltpu.SemaphoreType.DMA
    scratch = [
        pltpu.VMEM((2, ROWS), F32),
        pltpu.VMEM((2, COLS), F32),
        pltpu.VMEM((2, ROWS, COLS), BF16),
        pltpu.VMEM((2, ROWS, COLS), BF16),
        pltpu.VMEM((CHUNKS, WIDE, COLS), BF16),
        pltpu.VMEM((CHUNKS - LOCAL, WIDE, COLS), BF16),
        pltpu.VMEM((3, HALF, COLS), BF16),
        pltpu.VMEM((RINGS, 4, 2, VALUES, LANES), F32),
        pltpu.VMEM((RINGS, 3, 2, MESSAGE, LANES), BF16),
        pltpu.VMEM((RINGS, 3, 2, MESSAGE, LANES), BF16),
        pltpu.VMEM((LOCAL, 2, MESSAGE, LANES), BF16),
        pltpu.VMEM((LOCAL, 2, MESSAGE, LANES), BF16),
        pltpu.VMEM((LOCAL, 2, VALUES, LANES), F32),
        pltpu.VMEM((16, 8, LANES), F32),
        pltpu.VMEM((16, LANES), F32),
        pltpu.VMEM((16, LANES), F32),
        pltpu.VMEM((16, 16, LANES), F32),
        pltpu.VMEM((8, 16, LANES), F32),
        pltpu.VMEM((16, LANES), F32),
        pltpu.VMEM((16, LANES), F32),
        pltpu.VMEM((16, LANES), F32),
        pltpu.VMEM((16, LANES), F32),
        pltpu.VMEM((2, 8, LANES), F32),
        pltpu.VMEM((8, 8, LANES), F32),
        pltpu.VMEM((16, 8, LANES), F32),
        dma((2, PAIRS)), dma((2,)), dma((3,)), dma((STAT_SEMS,)), dma((STAT_SEMS,)),
        dma((3,)), dma((3,)), dma((3, 2)), dma((3, 2)), dma((3, 2)), dma((3, 2)), dma((4, 3)), dma((4, 3)),
        dma((CHUNKS,)), dma((CHUNKS,)), dma((RINGS, 3, 2)), dma((RINGS, 3, 2)),
        dma((LOCAL,)), dma((LOCAL,)),
    ]
    results = pl.pallas_call(
        kernel,
        out_shape=[
            pltpu.VMEM((PAIRS, BLOCK, UNIT), BF16),
            pltpu.VMEM((2, ROWS), F32),
            pltpu.VMEM((2, COLS), F32),
        ],
        in_specs=[hbm] * 5,
        out_specs=[vmem, vmem, vmem],
        scratch_shapes=scratch,
        compiler_params=pltpu.CompilerParams(
            collective_id=0, has_side_effects=True, vmem_limit_bytes=VMEM_LIMIT
        ),
        name="step",
    )(tokens, weights, gradients, row_factors, col_factors)
    return pl.pallas_call(
        writer,
        out_shape=[
            jax.ShapeDtypeStruct((BLOCK, ROWS), BF16),
            jax.ShapeDtypeStruct((2, ROWS), F32),
            jax.ShapeDtypeStruct((2, COLS), F32),
        ],
        in_specs=[vmem, vmem, vmem],
        out_specs=[hbm, hbm, hbm],
        scratch_shapes=[dma((PAIRS + 2,))],
        compiler_params=pltpu.CompilerParams(vmem_limit_bytes=2**20),
        name="write",
    )(*results)


def solution(mesh):
    torus = Mesh(mesh.devices.reshape(2, 4, 2, 2, 4), AXES)
    in_specs = (P(ROW, COL), P(None, ROW, COL), P(None, ROW, COL), P(None, ROW), P(None, COL))
    out_specs = (P(COL, ROW), P(None, ROW), P(None, COL))
    return jax.shard_map(local, mesh=torus, in_specs=in_specs, out_specs=out_specs, check_vma=False)
```

```python
import jax
import jax.numpy as jnp
from jax import lax
from jax.experimental import pallas as pl
from jax.experimental.pallas import tpu as pltpu
from jax.sharding import Mesh
from jax.sharding import PartitionSpec as P

D = 8192
FF = 14336
AXES = ("yl", "x", "c", "yh", "z")
ROW = ("yl", "x", "c")
COL = ("yh", "z")
F32 = jnp.float32
BF16 = jnp.bfloat16
BY_MESH = pl.DeviceIdType.MESH

decay_rate = 0.5
learn_rate = 0.01
clip_limit = 1.0
tiny_eps = 1e-30

ROWS = 896
COLS = 1024
UNIT = 128
PAIRS = ROWS // UNIT
CHUNKS = PAIRS
LOCAL = 4
RINGS = CHUNKS + LOCAL
VMEM_LIMIT = 67043328 - 464 * 1024
LAG = 2
WIDE = 2 * UNIT
VALUES = WIDE
MESSAGE = VALUES + 16
SPAN = 250.0
HALF_LOG = 125.0 * 0.6931471805599453
ORDER = [0, LOCAL, 1, LOCAL + 1] + list(range(2, LOCAL)) + list(range(LOCAL + 2, CHUNKS))
LANES = 128
TILES = COLS // LANES
HALF = 1024
BLOCK = 256

COL_SUMS, ROW_SUMS, SUM_XC, SUM_YZ = 0, 16, 24, 32
STAT_SEMS = 48


def spread(row):
    return jnp.transpose(jnp.broadcast_to(row, (LANES, LANES)))


def put_code(ref, v):
    v = v.reshape(-1, 8, LANES)
    top = jnp.maximum(jnp.max(jnp.abs(v), axis=0) * 1.004, 1e-30).astype(BF16)
    factor = SPAN / top.astype(F32)
    q = jnp.exp2(jnp.abs(v) * factor - SPAN / 2.0)
    ref[:VALUES] = jnp.where(v < 0.0, -q, q).reshape(VALUES, LANES).astype(BF16)
    ref[VALUES:] = jnp.concatenate([top, top], axis=0)


def get_code(ref):
    top = ref[VALUES:].astype(F32)[:8]
    q = ref[:VALUES].astype(F32).reshape(-1, 8, LANES)
    v = (jnp.log(jnp.abs(q)) + HALF_LOG) * (top * (1.0 / (2.0 * HALF_LOG)))
    return jnp.where(q < 0.0, -v, v).reshape(VALUES, LANES)


def kernel(
    tok, wgt, grd, row_old, col_old,
    hid, row_out, col_out,
    rowf, colf, g, w, wown, wpart, t, p, e, r, away, come, kept,
    colacc, colsrc, rowsrc, colin, rowin,
    rn, cn, a, b, sumsrc, sum_xc, sum_yz,
    g_sem, w_sem, in_sem, st_s, st_r, ty_s, ty_r, nx_s, nx_r, fx_s, fx_r, tc_s, tc_r,
    wy_s, wy_r, rs_s, rs_r, fy_s, fy_r,
):
    yl = lax.axis_index("yl")
    x = lax.axis_index("x")
    c = lax.axis_index("c")
    yh = lax.axis_index("yh")
    z = lax.axis_index("z")
    y = 2 * yh + yl

    def at_row(q):
        return {"yl": lax.div(q, 8), "x": lax.rem(lax.div(q, 2), 4), "c": lax.rem(q, 2)}

    def at_col(q):
        return {"yh": lax.div(q, 4), "z": lax.rem(q, 4)}

    def at_xc(q):
        return {"x": lax.div(q, 2), "c": lax.rem(q, 2)}

    def at_yz(q):
        return {"yh": lax.div(q, 8), "yl": lax.rem(lax.div(q, 4), 2), "z": lax.rem(q, 4)}

    in_row = yl * 8 + x * 2 + c
    in_col = yh * 4 + z
    in_xc = x * 2 + c
    in_yz = y * 4 + z
    x_next = lax.rem(x + 1, 4)
    x_prev = lax.rem(x + 3, 4)
    x_far = lax.rem(x + 2, 4)
    sibling = {"c": 1 - c}
    yh_peer = {"yh": 1 - yh}

    def remote(src, dst, s, q, device):
        return pltpu.make_async_remote_copy(
            src_ref=src, dst_ref=dst, send_sem=s, recv_sem=q,
            device_id=device, device_id_type=BY_MESH,
        )

    def g_copy(m, k):
        rows = pl.ds(k * UNIT, UNIT)
        return pltpu.make_async_copy(grd.at[m, rows], g.at[m, rows], g_sem.at[m, k])

    for m in range(2):
        for k in range(PAIRS):
            g_copy(m, k).start()
    w_copies = [pltpu.make_async_copy(wgt.at[m], w.at[m], w_sem.at[m]) for m in range(2)]

    def rows_of(q, core):
        return pl.ds(pl.multiple_of((q * 2 + core) * 128, 128), 128)

    mine = rows_of(x, c)
    same = yl == yh
    slots = [jnp.where(same, yh, 2), jnp.where(same, 2, yh), 1 - yh]
    tok_copy = pltpu.make_async_copy(tok, t.at[slots[0], mine], in_sem.at[0])
    tok_copy.start()
    factor_copies = [
        pltpu.make_async_copy(row_old, rowf, in_sem.at[1]),
        pltpu.make_async_copy(col_old, colf, in_sem.at[2]),
    ]
    for copy in factor_copies + w_copies:
        copy.start()

    barrier = pltpu.get_barrier_semaphore()
    peers = [at_row(lax.rem(in_row + d, 16)) for d in range(1, 16)]
    peers += [at_yz(lax.rem(in_yz + d, 16)) for d in range(1, 16)]
    for device in peers:
        pl.semaphore_signal(barrier, inc=1, device_id=device, device_id_type=BY_MESH)
    colacc[...] = jnp.zeros_like(colacc)
    rn[...] = jnp.ones_like(rn)
    rowsrc[...] = jnp.zeros_like(rowsrc)
    for m in range(2):
        def squares(k, carry):
            g_copy(m, k).wait()
            rows = pl.ds(pl.multiple_of(k * UNIT, UNIT), UNIT)
            total = jnp.zeros((UNIT, LANES), F32)
            for j in range(TILES):
                v = g[m, rows, j * LANES:(j + 1) * LANES].astype(F32)
                v = v * v
                total = total + v
                colacc[m * TILES + j] += jnp.sum(v.reshape(UNIT // 8, 8, LANES), axis=0)
            rowsrc[pl.ds(m * PAIRS + k, 1), :] = jnp.sum(
                jnp.transpose(total), axis=0, keepdims=True
            )
            return carry

        lax.fori_loop(0, PAIRS, squares, 0)
    colsrc[...] = jnp.sum(colacc[...], axis=1)
    pl.semaphore_wait(barrier, len(peers))

    sent = []

    def give(src, slots, place, n, me, device_of):
        for d in range(1, n):
            q = lax.rem(me + d, n)
            copy = remote(src, slots.at[me], st_s.at[place + q], st_r.at[place + me], device_of(q))
            copy.start()
            sent.append(copy)
        slots[me] = src[...]

    def arrive(src, slots, place, n, me, device_of):
        for d in range(1, n):
            q = lax.rem(me + d, n)
            remote(src, slots.at[q], st_s.at[place + q], st_r.at[place + q], device_of(q)).wait_recv()

    def take(src, slots, place, n, me, device_of):
        arrive(src, slots, place, n, me, device_of)
        total = slots[0]
        for q in range(1, n):
            total = total + slots[q]
        return total

    give(rowsrc, rowin, ROW_SUMS, 8, in_col, at_col)
    give(colsrc, colin, COL_SUMS, 16, in_row, at_row)

    def near(f, side):
        rows = mine
        return remote(
            t.at[slots[f], rows], t.at[slots[f], rows], nx_s.at[f, side], nx_r.at[f, side],
            {"x": x_next if side == 0 else x_prev},
        )

    def near_in(f, side):
        rows = rows_of(x_prev if side == 0 else x_next, c)
        return remote(
            t.at[slots[f], rows], t.at[slots[f], rows], nx_s.at[f, side], nx_r.at[f, side],
            {"x": x_next if side == 0 else x_prev},
        )

    def half_rows(q, side):
        return pl.ds(pl.multiple_of((q * 2 + c) * 128 + 64 * side, 64), 64)

    def onward(f, side):
        rows = half_rows(x_prev if side == 0 else x_next, side)
        return remote(
            t.at[slots[f], rows], t.at[slots[f], rows], fx_s.at[f, side], fx_r.at[f, side],
            {"x": x_next if side == 0 else x_prev},
        )

    def onward_in(f, side):
        rows = half_rows(x_far, side)
        return remote(
            t.at[slots[f], rows], t.at[slots[f], rows], fx_s.at[f, side], fx_r.at[f, side],
            {"x": x_next if side == 0 else x_prev},
        )

    def to_sibling(q, f):
        rows = rows_of(q, c)
        return remote(t.at[slots[f], rows], t.at[slots[f], rows], tc_s.at[q, f], tc_r.at[q, f], sibling)

    def from_sibling(q, f):
        rows = rows_of(q, 1 - c)
        return remote(t.at[slots[f], rows], t.at[slots[f], rows], tc_s.at[q, f], tc_r.at[q, f], sibling)

    pair_send = remote(t.at[slots[0], mine], t.at[slots[0], mine], ty_s.at[0], ty_r.at[0], {"yl": 1 - yl})
    pair_in = remote(t.at[slots[1], mine], t.at[slots[1], mine], ty_s.at[0], ty_r.at[0], {"yl": 1 - yl})
    across_send = remote(
        t.at[slots[0], mine], t.at[yh, mine], ty_s.at[1], ty_r.at[1], {"yl": 1 - yl, "yh": 1 - yh}
    )
    across_in = remote(
        t.at[slots[2], mine], t.at[slots[2], mine], ty_s.at[1], ty_r.at[1], {"yl": 1 - yl, "yh": 1 - yh}
    )
    far_send = remote(t.at[slots[0], mine], t.at[yh, mine], ty_s.at[2], ty_r.at[2], yh_peer)
    far_in = remote(t.at[slots[2], mine], t.at[slots[2], mine], ty_s.at[2], ty_r.at[2], yh_peer)

    def share(f):
        for side in range(2):
            near(f, side).start()
        to_sibling(x, f).start()

    def pass_on(f):
        for side in range(2):
            near_in(f, side).wait_recv()
            onward(f, side).start()
        to_sibling(x_prev, f).start()
        to_sibling(x_next, f).start()

    def complete(f):
        for side in range(2):
            onward_in(f, side).wait_recv()
        to_sibling(x_far, f).start()

    def complete_sibling(f):
        for q in (x, x_prev, x_next, x_far):
            from_sibling(q, f).wait_recv()

    tok_copy.wait()
    pair_send.start()

    @pl.when(jnp.logical_not(same))
    def _():
        across_send.start()
        far_send.start()

    share(0)
    for copy in factor_copies:
        copy.wait()

    for copy in w_copies:
        copy.wait()
    sumsrc[...] = jnp.zeros_like(sumsrc)

    row_total = take(rowsrc, rowin, ROW_SUMS, 8, in_col, at_col)
    for m in range(2):
        for k in range(PAIRS):
            i = m * PAIRS + k
            rn[i:i + 1] = decay_rate * rowf[m:m + 1, k * UNIT:(k + 1) * UNIT] + (1.0 - decay_rate) * (
                row_total[i:i + 1] / D + tiny_eps
            )
            row_out[m:m + 1, k * UNIT:(k + 1) * UNIT] = rn[i:i + 1]
    col_total = take(colsrc, colin, COL_SUMS, 16, in_row, at_row)
    for m in range(2):
        for j in range(TILES):
            i = m * TILES + j
            cn[i:i + 1] = decay_rate * colf[m:m + 1, j * LANES:(j + 1) * LANES] + (1.0 - decay_rate) * (
                col_total[i:i + 1] / FF + tiny_eps
            )
            col_out[m:m + 1, j * LANES:(j + 1) * LANES] = cn[i:i + 1]

    a[...] = 1.0 / rn[...]
    b[...] = 1.0 / cn[...]
    for m in range(2):
        def norms(k, carry):
            rows = pl.ds(pl.multiple_of(k * UNIT, UNIT), UNIT)
            total = jnp.zeros((UNIT, LANES), F32)
            for j in range(TILES):
                v = g[m, rows, j * LANES:(j + 1) * LANES].astype(F32)
                total = total + v * v * b[m * TILES + j:m * TILES + j + 1]
            total = total * spread(a[pl.ds(m * PAIRS + k, 1), :])
            return carry + jnp.sum(total.reshape(UNIT // 8, 8, LANES), axis=0)

        parts = lax.fori_loop(0, PAIRS, norms, jnp.zeros((8, LANES), F32))
        sumsrc[0, m:m + 1] = jnp.sum(parts, axis=0, keepdims=True)
        sumsrc[0, 2 + m:3 + m] = jnp.sum(rn[m * PAIRS:(m + 1) * PAIRS], axis=0, keepdims=True)

    give(sumsrc.at[0], sum_xc, SUM_XC, 8, in_xc, at_xc)
    pass_on(0)
    pair_in.wait_recv()
    share(1)
    sumsrc[1] = take(sumsrc.at[0], sum_xc, SUM_XC, 8, in_xc, at_xc)
    give(sumsrc.at[1], sum_yz, SUM_YZ, 16, in_yz, at_yz)
    complete(0)
    total = take(sumsrc.at[1], sum_yz, SUM_YZ, 16, in_yz, at_yz)

    for m in range(2):
        row_mean = jnp.sum(total[2 + m:3 + m], axis=1, keepdims=True) / (8.0 * FF)
        norm_total = jnp.sum(total[m:m + 1], axis=1, keepdims=True) * row_mean
        clip_scale = jnp.maximum(1.0, jnp.sqrt(norm_total / (FF * D)) / clip_limit)
        scale = learn_rate * jnp.sqrt(row_mean) / clip_scale
        a[m * PAIRS:(m + 1) * PAIRS] = scale / jnp.sqrt(rn[m * PAIRS:(m + 1) * PAIRS])
    b[...] = 1.0 / jnp.sqrt(cn[...])

    def weight_send(k):
        return remote(wown.at[k], wpart.at[k - LOCAL], wy_s.at[k], wy_r.at[k], yh_peer)

    def update(i, carry):
        k = ORDER[-1]
        for q in range(CHUNKS - 1):
            k = jnp.where(i == q, ORDER[q], k)
        rows = pl.ds(pl.multiple_of(k * UNIT, UNIT), UNIT)
        for m in range(2):
            factor = spread(a[pl.ds(m * PAIRS + k, 1), :])
            for j in range(TILES):
                cols = slice(j * LANES, (j + 1) * LANES)
                step = g[m, rows, cols].astype(F32) * factor * b[m * TILES + j:m * TILES + j + 1]
                wown[k, m * UNIT:(m + 1) * UNIT, cols] = (w[m, rows, cols].astype(F32) - step).astype(BF16)

        @pl.when(k >= LOCAL)
        def _():
            weight_send(k).start()

        return carry

    lax.fori_loop(0, 1, update, 0)
    complete_sibling(0)

    right = lax.rem(z + 1, 4)
    left = lax.rem(z + 3, 4)

    def block_of(side, s):
        return lax.rem(z + 3 - s, 4) if side == 0 else lax.rem(z + 1 + s, 4)

    def ring_copy(n, s, side):
        target = right if side == 0 else left
        return remote(
            e.at[n, s, side], r.at[n, s, side],
            rs_s.at[n, s, side], rs_r.at[n, s, side], {"z": target},
        )

    def times(block, slot, weights):
        tokens = t[slot, pl.ds(pl.multiple_of(block * BLOCK, BLOCK), BLOCK), :]
        return lax.dot_general(
            tokens, weights[...], (((1,), (1,)), ((), ())), preferred_element_type=F32
        )

    def arrange(v):
        parts = []
        for side in range(2):
            rows = slice(side * (BLOCK // 2), (side + 1) * (BLOCK // 2))
            parts.append(jnp.concatenate([v[rows, :UNIT], v[rows, UNIT:]], axis=0))
        return parts

    def begin(n, d, parts):
        if d in (3, 1):
            side = 0 if d == 3 else 1
            put_code(e.at[n, 0, side], parts[side])
            ring_copy(n, 0, side).start()

    def local_products(n):
        k = jnp.where(n < LOCAL, n, n - LOCAL)
        slot = jnp.where(n < LOCAL, slots[0], slots[1])
        for d in (3, 1, 2, 0):
            block = lax.rem(z + d, 4)
            parts = arrange(times(block, slot, wown.at[k]))
            for side in range(2):
                p[n, block, side] = parts[side]
            begin(n, d, parts)

    def own_products(n):
        for d in (3, 1, 2, 0):
            block = lax.rem(z + d, 4)
            parts = arrange(times(block, yh, wown.at[n - LOCAL]))
            for side in range(2):
                p[n, block, side] = parts[side]

    def other_products(n):
        for d in (3, 1, 2, 0):
            block = lax.rem(z + d, 4)
            parts = arrange(times(block, 1 - yh, wpart.at[n - 2 * LOCAL]))
            for side in range(2):
                parts[side] = parts[side] + p[n, block, side]
                p[n, block, side] = parts[side]
            begin(n, d, parts)

    def ring_step(n, s):
        for side in range(2):
            ring_copy(n, s - 1, side).wait_recv()
            put_code(e.at[n, s, side], p[n, block_of(side, s), side] + get_code(r.at[n, s - 1, side]))
            ring_copy(n, s, side).start()

    def hidden(k, side, v):
        gate = v[:UNIT]
        up = v[UNIT:]
        rows = slice(side * (BLOCK // 2), (side + 1) * (BLOCK // 2))
        hid[k, rows] = (gate / (1.0 + jnp.exp(-gate)) * up).astype(BF16)

    def final_send(n):
        return remote(away.at[n], come.at[n], fy_s.at[n], fy_r.at[n], yh_peer)

    def leaves(n):
        return (jnp.logical_not(same) & (n < LOCAL)) | (same & (n >= LOCAL) & (n < 2 * LOCAL))

    def finish(n):
        for side in range(2):
            ring_copy(n, 2, side).wait_recv()
            v = p[n, z, side] + get_code(r.at[n, 2, side])

            @pl.when(leaves(n))
            def _():
                put_code(away.at[lax.rem(n, LOCAL), side], v)

            @pl.when(jnp.logical_not(leaves(n)) & (n < 2 * LOCAL))
            def _():
                kept[lax.rem(n, LOCAL), side] = v

            @pl.when(n >= 2 * LOCAL)
            def _():
                hidden(n - LOCAL, side, v)

        @pl.when(leaves(n))
        def _():
            final_send(lax.rem(n, LOCAL)).start()

    def work(n, carry):
        @pl.when(n < 2 * LOCAL)
        def _():
            local_products(n)

        @pl.when((n >= 2 * LOCAL) & (n < RINGS))
        def _():
            own_products(n)

        @pl.when(n < PAIRS - 3)
        def _():
            lax.fori_loop(jnp.where(n == 0, 1, n + 3), n + 4, update, 0)

        for s in (1, 2):
            @pl.when((n >= s * LAG) & (n < RINGS + s * LAG))
            def _():
                ring_step(n - s * LAG, s)

        @pl.when(n >= 3 * LAG)
        def _():
            finish(n - 3 * LAG)

        @pl.when(n == 0)
        def _():
            pass_on(1)

        @pl.when(n == 4)
        def _():
            @pl.when(same)
            def _():
                far_in.wait_recv()

            @pl.when(jnp.logical_not(same))
            def _():
                across_in.wait_recv()

            share(2)

        @pl.when(n == LOCAL + 2)
        def _():
            pass_on(2)

        @pl.when(n == LOCAL - 1)
        def _():
            complete(1)
            complete_sibling(1)

        @pl.when(n == 2 * LOCAL)
        def _():
            complete(2)
            complete_sibling(2)

        @pl.when((n >= 2 * LOCAL) & (n < RINGS))
        def _():
            weight_send(n - LOCAL).wait_recv()
            other_products(n)

        return carry

    lax.fori_loop(0, RINGS + 3 * LAG, work, 0)

    def last(n, carry):
        final_send(n).wait_recv()
        for side in range(2):
            hidden(n, side, kept[n, side] + get_code(come.at[n, side]))
        return carry

    lax.fori_loop(0, LOCAL, last, 0)

    for copy in sent:
        copy.wait_send()
    pair_send.wait_send()

    @pl.when(jnp.logical_not(same))
    def _():
        across_send.wait_send()
        far_send.wait_send()

    for f in range(3):
        for side in range(2):
            near(f, side).wait_send()
            onward(f, side).wait_send()
        for q in range(4):
            to_sibling(q, f).wait_send()

    def drain(n, carry):
        @pl.when(n >= 2 * LOCAL)
        def _():
            weight_send(n - LOCAL).wait_send()

        @pl.when(n < LOCAL)
        def _():
            final_send(n).wait_send()

        for s in range(3):
            for side in range(2):
                ring_copy(n, s, side).wait_send()
        return carry

    lax.fori_loop(0, RINGS, drain, 0)


def writer(hid, row_new, col_new, hid_out, row_out, col_out, sem):
    copies = [
        pltpu.make_async_copy(hid.at[k], hid_out.at[:, k * UNIT:(k + 1) * UNIT], sem.at[k])
        for k in range(PAIRS)
    ]
    copies += [
        pltpu.make_async_copy(row_new, row_out, sem.at[PAIRS]),
        pltpu.make_async_copy(col_new, col_out, sem.at[PAIRS + 1]),
    ]
    for copy in copies:
        copy.start()
    for copy in copies:
        copy.wait()


def local(tokens, weights, gradients, row_factors, col_factors):
    vmem = pl.BlockSpec(memory_space=pltpu.VMEM)
    hbm = pl.BlockSpec(memory_space=pl.ANY)
    dma = pltpu.SemaphoreType.DMA
    scratch = [
        pltpu.VMEM((2, ROWS), F32),
        pltpu.VMEM((2, COLS), F32),
        pltpu.VMEM((2, ROWS, COLS), BF16),
        pltpu.VMEM((2, ROWS, COLS), BF16),
        pltpu.VMEM((CHUNKS, WIDE, COLS), BF16),
        pltpu.VMEM((CHUNKS - LOCAL, WIDE, COLS), BF16),
        pltpu.VMEM((3, HALF, COLS), BF16),
        pltpu.VMEM((RINGS, 4, 2, VALUES, LANES), F32),
        pltpu.VMEM((RINGS, 3, 2, MESSAGE, LANES), BF16),
        pltpu.VMEM((RINGS, 3, 2, MESSAGE, LANES), BF16),
        pltpu.VMEM((LOCAL, 2, MESSAGE, LANES), BF16),
        pltpu.VMEM((LOCAL, 2, MESSAGE, LANES), BF16),
        pltpu.VMEM((LOCAL, 2, VALUES, LANES), F32),
        pltpu.VMEM((16, 8, LANES), F32),
        pltpu.VMEM((16, LANES), F32),
        pltpu.VMEM((16, LANES), F32),
        pltpu.VMEM((16, 16, LANES), F32),
        pltpu.VMEM((8, 16, LANES), F32),
        pltpu.VMEM((16, LANES), F32),
        pltpu.VMEM((16, LANES), F32),
        pltpu.VMEM((16, LANES), F32),
        pltpu.VMEM((16, LANES), F32),
        pltpu.VMEM((2, 8, LANES), F32),
        pltpu.VMEM((8, 8, LANES), F32),
        pltpu.VMEM((16, 8, LANES), F32),
        dma((2, PAIRS)), dma((2,)), dma((3,)), dma((STAT_SEMS,)), dma((STAT_SEMS,)),
        dma((3,)), dma((3,)), dma((3, 2)), dma((3, 2)), dma((3, 2)), dma((3, 2)), dma((4, 3)), dma((4, 3)),
        dma((CHUNKS,)), dma((CHUNKS,)), dma((RINGS, 3, 2)), dma((RINGS, 3, 2)),
        dma((LOCAL,)), dma((LOCAL,)),
    ]
    results = pl.pallas_call(
        kernel,
        out_shape=[
            pltpu.VMEM((PAIRS, BLOCK, UNIT), BF16),
            pltpu.VMEM((2, ROWS), F32),
            pltpu.VMEM((2, COLS), F32),
        ],
        in_specs=[hbm] * 5,
        out_specs=[vmem, vmem, vmem],
        scratch_shapes=scratch,
        compiler_params=pltpu.CompilerParams(
            collective_id=0, has_side_effects=True, vmem_limit_bytes=VMEM_LIMIT
        ),
        name="step",
    )(tokens, weights, gradients, row_factors, col_factors)
    return pl.pallas_call(
        writer,
        out_shape=[
            jax.ShapeDtypeStruct((BLOCK, ROWS), BF16),
            jax.ShapeDtypeStruct((2, ROWS), F32),
            jax.ShapeDtypeStruct((2, COLS), F32),
        ],
        in_specs=[vmem, vmem, vmem],
        out_specs=[hbm, hbm, hbm],
        scratch_shapes=[dma((PAIRS + 2,))],
        compiler_params=pltpu.CompilerParams(vmem_limit_bytes=2**20),
        name="write",
    )(*results)


def solution(mesh):
    torus = Mesh(mesh.devices.reshape(2, 4, 2, 2, 4), AXES)
    in_specs = (P(ROW, COL), P(None, ROW, COL), P(None, ROW, COL), P(None, ROW), P(None, COL))
    out_specs = (P(COL, ROW), P(None, ROW), P(None, COL))
    return jax.shard_map(local, mesh=torus, in_specs=in_specs, out_specs=out_specs, check_vma=False)
```
